32 devices in a mesh: group: 8 (over z, x), rad: 4 (over y, core).
Axes of the slice: x: 2, y: 2, z: 4, core: 2. Of those that a mesh axis runs over, the one named last changes fastest.
Arguments:
- source_term: float32 [32, 128, 1024], P('group', 'rad'), may hold values from -6 to 6
- initial_guess: float32 [32, 128, 1024], P('group', 'rad'), may hold values from -3 to 3
- metric: float32 [3, 8, 32, 256], P(None, 'group', 'rad'), may hold values from 0.5 to 4
Outputs:
- solution: float32 [32, 128, 1024], P('group', 'rad')
- residual: float32 [32, 128, 1024], P('group', 'rad')
The draws below stay inside these ranges and needn't reach their ends.
All inputs are finite; a program needn't handle non-finite values.
Results may differ from the reference program's by a relative error of at most 0.00025.
Values sent between devices are 32-bit elements; how exact they have to be, the bound alone decides.
No kernel may reach another device: no remote copies, remote signals or barrier semaphores. Data moves between devices by JAX's collectives and lax.ppermute only.
A program may use at most 128 MiB of HBM per device.

```python
import math
import jax
import jax.numpy as jnp
import numpy as np
from jax import lax

EY = 256
ITERS = 3
NEX = 8
NER = 32
NX = 32
NR = 128
NY = 1024


def block_levels(key, extent, shards, least, high):
    def one(position, blocks):
        steps = jax.random.uniform(jax.random.fold_in(jax.random.fold_in(key, 6), position), (blocks,), jnp.float32, least / len(shards), high / len(shards))
        return jnp.repeat(jnp.exp(steps), extent[position] // blocks).reshape((-1,) + (1,) * (len(extent) - position - 1))

    level = one(*shards[0])
    for cut in shards[1:]:
        level = level * one(*cut)
    return level


def gaussian(key, shape, width, reach, pieces=(), held_as=jnp.bfloat16):
    values = width * jax.random.normal(key, shape, jnp.float32)
    if pieces:
        values = values * block_levels(key, shape, pieces, -0.22, 0.18)
    return jnp.clip(values, -reach, reach).astype(held_as)


def setup_inputs(seed: int = 0) -> dict:
    streams_of = jax.random.split(jax.random.key(seed), 4)
    source_term = gaussian(streams_of[0], (NX, NR, NY), 1.0, 6.0, ((0, 8), (1, 4)), jnp.float32)
    initial_guess = gaussian(streams_of[1], (NX, NR, NY), 0.5, 3.0, ((0, 8), (1, 4)), jnp.float32)
    metric = jnp.clip(jnp.exp(math.log(4.0) - 2.0794415 * jax.random.uniform(streams_of[2], (3, NEX, NER, EY), jnp.float32) ** block_levels(streams_of[2], (3, NEX, NER, EY), ((1, 8), (2, 4)), -0.2, 0.2)), 0.5, 4.0)
    return dict(source_term=source_term, initial_guess=initial_guess, metric=metric)


def gll_tables():
    root = math.sqrt(3.0 / 7.0)
    points = np.array([-1.0, -root, 0.0, root, 1.0])
    weights = np.array([0.1, 49.0 / 90.0, 32.0 / 45.0, 49.0 / 90.0, 0.1])
    factor = np.array([np.prod([points[a] - points[m] for m in range(5) if m != a]) for a in range(5)])
    derivative = np.zeros((5, 5))
    for p in range(5):
        for a in range(5):
            if p == a:
                derivative[p, a] = np.sum([1.0 / (points[a] - points[m]) for m in range(5) if m != a])
            else:
                derivative[p, a] = factor[p] / (factor[a] * (points[p] - points[a]))
    return (jnp.asarray(derivative, jnp.float32), jnp.asarray(weights, jnp.float32))

def take_every(values, first, number, dim_axis):
    return lax.slice_in_dim(values, first, first + 4 * (number - 1) + 1, 4, dim_axis)

def to_elements(extended, count_x, count_r, count_y):
    layers = [take_every(extended, k, count_y, 2) for k in range(4)]
    layers.append(jnp.roll(layers[0], -1, axis=2))
    stacked = jnp.stack(layers, 0)
    across = jnp.stack([take_every(stacked, i, count_x, 1) for i in range(5)], 0)
    return jnp.stack([take_every(across, j, count_r, 3) for j in range(5)], 1)

def spread(values, low_pad, high_pad, dim_axis):
    config = [(0, 0, 0)] * values.ndim
    config[dim_axis] = (low_pad, high_pad, 3)
    return lax.pad(values, jnp.zeros((), values.dtype), config)

def from_elements(result):
    along_r = spread(result[:, 0], 0, 4, 3)
    for j in range(1, 5):
        along_r = along_r + spread(result[:, j], j, 4 - j, 3)
    along_x = spread(along_r[0], 0, 4, 1)
    for i in range(1, 5):
        along_x = along_x + spread(along_r[i], i, 4 - i, 1)
    first = along_x[0] + jnp.roll(along_x[4], 1, axis=2)
    total = spread(first, 0, 3, 2)
    for k in range(1, 4):
        total = total + spread(along_x[k], k, 3 - k, 2)
    return total

def apply_elements(elements, metric):
    derivative, weights = gll_tables()
    derivative = derivative.astype(elements.dtype)
    weights = weights.astype(elements.dtype)
    quad_weight = (weights[:, None, None] * weights[None, :, None] * weights[None, None, :]).reshape(5, 5, 5, 1, 1, 1)
    high = lax.Precision.HIGHEST
    grad_x = jnp.einsum('pa,abcxyz->pbcxyz', derivative, elements, precision=high)
    result_sum = jnp.einsum('pa,pbcxyz->abcxyz', derivative, grad_x * quad_weight * metric[0], precision=high)
    grad_r = jnp.einsum('qb,abcxyz->aqcxyz', derivative, elements, precision=high)
    result_sum = result_sum + jnp.einsum('qb,aqcxyz->abcxyz', derivative, grad_r * quad_weight * metric[1], precision=high)
    grad_y = jnp.einsum('sc,abcxyz->absxyz', derivative, elements, precision=high)
    result_sum = result_sum + jnp.einsum('sc,absxyz->abcxyz', derivative, grad_y * quad_weight * metric[2], precision=high)
    return result_sum

def element_diagonal(metric):
    derivative, weights = gll_tables()
    derivative = derivative.astype(metric.dtype)
    weights = weights.astype(metric.dtype)
    squared = lax.optimization_barrier(jnp.sum(derivative * derivative * weights[:, None], axis=0))
    term_x = (squared[:, None, None] * weights[None, :, None] * weights[None, None, :]).reshape(5, 5, 5, 1, 1, 1)
    term_r = (weights[:, None, None] * squared[None, :, None] * weights[None, None, :]).reshape(5, 5, 5, 1, 1, 1)
    term_y = (weights[:, None, None] * weights[None, :, None] * squared[None, None, :]).reshape(5, 5, 5, 1, 1, 1)
    return term_x * metric[0] + term_r * metric[1] + term_y * metric[2]

def fold_cycle(raw):
    last_x = raw.shape[0] - 1
    last_r = raw.shape[1] - 1
    interior = raw[:last_x, :last_r]
    return jnp.concatenate([interior[0:1] + raw[last_x:, :last_r], interior[1:]], 0)

def operate(field, metric):
    extended = jnp.concatenate([field, field[0:1]], 0)
    extended = jnp.concatenate([extended, jnp.zeros_like(extended[:, 0:1])], 1)
    elements = to_elements(extended, metric.shape[1], metric.shape[2], metric.shape[3])
    return fold_cycle(from_elements(apply_elements(elements, metric)))

def reference(source_term, initial_guess, metric):
    diagonal = fold_cycle(from_elements(element_diagonal(metric)))
    scaling = 1.0 / diagonal
    residual = source_term - operate(initial_guess, metric)
    solution = initial_guess
    smoothed = scaling * residual
    direction = smoothed
    weighted_norm = jnp.sum(residual * smoothed)
    for iteration in range(ITERS):
        applied = operate(direction, metric)
        step_size = weighted_norm / jnp.sum(direction * applied)
        solution = solution + step_size * direction
        residual = residual - step_size * applied
        if iteration + 1 < ITERS:
            smoothed = scaling * residual
            next_norm = jnp.sum(residual * smoothed)
            direction = smoothed + next_norm / weighted_norm * direction
            weighted_norm = next_norm
    return (solution, residual)
```

```python
import math

import jax
import jax.numpy as jnp
import numpy as np
from jax import lax
from jax.experimental import pallas as pl
from jax.experimental.pallas import tpu as pltpu
from jax.sharding import PartitionSpec as P

F32 = jnp.float32
BF16 = jnp.bfloat16
LANES = 128
ROWS = 8
SHIFT = 1.145
DOTS = 6


def gll_tables():
    root = math.sqrt(3.0 / 7.0)
    points = np.array([-1.0, -root, 0.0, root, 1.0])
    weights = np.array([0.1, 49.0 / 90.0, 32.0 / 45.0, 49.0 / 90.0, 0.1])
    factor = np.array(
        [np.prod([points[a] - points[m] for m in range(5) if m != a]) for a in range(5)]
    )
    derivative = np.zeros((5, 5))
    for p in range(5):
        for a in range(5):
            if p == a:
                derivative[p, a] = np.sum(
                    [1.0 / (points[a] - points[m]) for m in range(5) if m != a]
                )
            else:
                derivative[p, a] = factor[p] / (factor[a] * (points[p] - points[a]))
    return derivative, weights


DERIVATIVE, WEIGHTS = gll_tables()
STIFF = DERIVATIVE.T @ np.diag(WEIGHTS) @ DERIVATIVE
K = [[float(v) for v in row] for row in STIFF]
W = [float(v) for v in WEIGHTS]


def line_operator(u):
    u0, u1, u2, u3, u4 = u
    s = u0 if u4 is None else u0 + u4
    o0 = u0 if u4 is None else u0 - u4
    t = u1 + u3
    o1 = u1 - u3
    q = u2 + u2
    d0 = s - q
    d1 = t - q
    e0 = (0.5 * (K[0][0] + K[0][4])) * d0 + (0.5 * (K[0][1] + K[0][3])) * d1
    e1 = (0.5 * (K[1][0] + K[1][4])) * d0 + (0.5 * (K[1][1] + K[1][3])) * d1
    p0 = (0.5 * (K[0][0] - K[0][4])) * o0 + (0.5 * (K[0][1] - K[0][3])) * o1
    p1 = (0.5 * (K[1][0] - K[1][4])) * o0 + (0.5 * (K[1][1] - K[1][3])) * o1
    e = e0 + e1
    return e0 + p0, e1 + p1, -(e + e), e1 - p1, e0 - p0


def last_row(u):
    return K[4][0] * u[0] + K[4][1] * u[1] + K[4][2] * u[2] + K[4][3] * u[3]


class Shape:
    def __init__(self, count_r, count_y):
        self.rows = count_r
        self.halves = count_y // LANES
        self.wide = 4 * LANES

    def row(self, index):
        return pl.ds(self.rows * index, self.rows)

    def lane(self, h, c):
        return pl.ds(self.wide * h + LANES * c, LANES)

    def half(self, h):
        return pl.ds(LANES * h, LANES)


def row_index(g):
    return lax.broadcasted_iota(jnp.int32, (g.rows, LANES), 0)


def lane_index(g):
    return lax.broadcasted_iota(jnp.int32, (g.rows, LANES), 1)


def next_lane(parts, lanes):
    rolled = [pltpu.roll(p, LANES - 1, 1) for p in parts]
    n = len(parts)
    return [jnp.where(lanes == LANES - 1, rolled[(h + 1) % n], rolled[h]) for h in range(n)]


def prev_lane(parts, lanes):
    rolled = [pltpu.roll(p, 1, 1) for p in parts]
    n = len(parts)
    return [jnp.where(lanes == 0, rolled[(h - 1) % n], rolled[h]) for h in range(n)]


def next_row(g, value, rows, last):
    return jnp.where(rows == g.rows - 1, last, pltpu.roll(value, g.rows - 1, 0))


def prev_row(value, rows, first):
    return jnp.where(rows == 0, first, pltpu.roll(value, 1, 0))


def permutation():
    source = lax.broadcasted_iota(jnp.int32, (4 * LANES, 4 * LANES), 0)
    target = lax.broadcasted_iota(jnp.int32, (4 * LANES, 4 * LANES), 1)
    wanted = (target % LANES) * 4 + target // LANES
    return jnp.where(source == wanted, 1.0, 0.0).astype(BF16)


def exact_dot(values, matrix, dims):
    one = values.astype(BF16)
    rest = values - one.astype(F32)
    two = rest.astype(BF16)
    three = (rest - two.astype(F32)).astype(BF16)
    dot = lambda v: lax.dot_general(v, matrix, (dims, ((), ())), preferred_element_type=F32)
    return (dot(one) + dot(two)) + dot(three)


def local_apply(g, u_ref, cx, cxp, cr, crp, cy, v_ref):
    rows = row_index(g)
    lanes = lane_index(g)
    for ab in range(16):
        u = [[u_ref[g.row(ab), g.lane(h, c)] for c in range(4)] for h in range(g.halves)]
        fifth = next_lane([u[h][0] for h in range(g.halves)], lanes)
        ends = []
        outs = []
        for h in range(g.halves):
            coef = cy[g.row(ab), g.half(h)]
            r = line_operator(u[h] + [fifth[h]])
            outs.append([coef * r[c] for c in range(4)])
            ends.append(coef * r[4])
        ends = prev_lane(ends, lanes)
        for h in range(g.halves):
            outs[h][0] = outs[h][0] + ends[h]
            for c in range(4):
                v_ref[g.row(ab), g.lane(h, c)] = outs[h][c]
    for h in range(g.halves):
        for c in range(4):
            at = g.lane(h, c)
            u = [[u_ref[g.row(4 * a + b), at] for b in range(4)] for a in range(4)]
            v = [[v_ref[g.row(4 * a + b), at] for b in range(4)] for a in range(4)]
            for b in range(4):
                coef = cx[g.row(b), at]
                r = line_operator([u[a][b] for a in range(4)] + [None])
                for a in range(4):
                    v[a][b] = v[a][b] + coef * r[a]
                v[0][b] = v[0][b] + K[4][4] * (cxp[g.row(b), at] * u[0][b])
            for a in range(4):
                coef = cr[g.row(a), at]
                r = line_operator(u[a] + [next_row(g, u[a][0], rows, 0.0)])
                for b in range(4):
                    v[a][b] = v[a][b] + coef * r[b]
                v[a][0] = v[a][0] + prev_row(coef * r[4], rows, 0.0)
                v[a][0] = v[a][0] + K[4][4] * (crp[g.row(a), at] * u[a][0])
            for a in range(4):
                for b in range(4):
                    v_ref[g.row(4 * a + b), at] = v[a][b]


def add_halo(g, v, coef_x, coef_r, above_x, below_x, above_r, below_r, rows):
    for b in range(4):
        reach = coef_x[b] * above_x[b]
        for a in range(4):
            v[a][b] = v[a][b] + K[a][4] * reach
        v[0][b] = v[0][b] + below_x[b]
    for a in range(4):
        reach = jnp.where(rows == g.rows - 1, coef_r[a] * above_r[a], 0.0)
        for b in range(4):
            v[a][b] = v[a][b] + K[b][4] * reach
        v[a][0] = v[a][0] + jnp.where(rows == 0, below_r[a], 0.0)


def send_planes(g, z, at, h, c, coef_x, coef_r, even_x, even_r, out):
    p1, p2, p3, p4 = out
    for b in range(4):
        down = z[0][b]
        up = coef_x[b] * last_row([z[a][b] for a in range(4)])
        p1[g.row(b), at] = jnp.where(even_x, up, down)
        p2[g.row(b), at] = jnp.where(even_x, down, up)
    for a in range(4):
        down = z[a][0][0:1]
        up = (coef_r[a] * last_row(z[a]))[g.rows - 1 :]
        p3[pl.ds(4 * a + c, 1), g.half(h)] = jnp.where(even_r, up, down)
        p4[pl.ds(4 * a + c, 1), g.half(h)] = jnp.where(even_r, down, up)


def positions():
    ix = lax.axis_index("group")
    ir = lax.axis_index("rad")
    top = ir == lax.axis_size("rad") - 1
    return ix % 2 == 0, ir % 2 == 0, ir == 0, top


def start_kernel(g):
    def body(x_hbm, m_hbm, x_ref, m_ref, p1, p2, p3, p4, corner, sems):
        copies = [pltpu.make_async_copy(x_hbm.at[a], x_ref.at[a], sems.at[a]) for a in range(4)]
        copies.append(pltpu.make_async_copy(m_hbm, m_ref, sems.at[4]))
        for copy in copies:
            copy.start()
        even_x, even_r, _, _ = positions()
        last = g.rows - 1
        n = 4 * g.rows
        span = LANES * g.halves
        corner[...] = jnp.zeros_like(corner)
        p3[...] = jnp.zeros_like(p3)
        p4[...] = jnp.zeros_like(p4)
        for copy in copies:
            copy.wait()
        down = x_ref[0]
        up = last_row([x_ref[a] for a in range(4)])
        p1[0:n] = jnp.where(even_x, up, down)
        p2[0:n] = jnp.where(even_x, down, up)
        for k in range(3):
            m = m_ref[k, 0]
            p1[pl.ds(n, g.rows), pl.ds(span * k, span)] = m
            p2[pl.ds(n, g.rows), pl.ds(span * k, span)] = m
            edge = m[last:]
            corner[pl.ds(k, 1), :] = edge
            p3[pl.ds(4, 1), pl.ds(span * k, span)] = edge
            p4[pl.ds(4, 1), pl.ds(span * k, span)] = edge
        p1[pl.ds(n, g.rows), pl.ds(span * 3, span)] = m
        p2[pl.ds(n, g.rows), pl.ds(span * 3, span)] = m
        for a in range(4):
            down = x_ref[a, 0:1]
            up = last_row([x_ref[a, pl.ds(4 * last + b, 1)] for b in range(4)])
            p3[pl.ds(a, 1)] = jnp.where(even_r, up, down)
            p4[pl.ds(a, 1)] = jnp.where(even_r, down, up)

    return body


def arrange_kernel(g):
    def body(x_ref, s_ref, xd, sd, matrix_ref, buffer):
        matrix = permutation()
        matrix_ref[...] = matrix
        for source, target in ((x_ref, xd), (s_ref, sd)):
            for h in range(g.halves):
                part = source[:, :, pl.ds(g.wide * h, g.wide)].reshape(16 * g.rows, g.wide)
                part = exact_dot(part, matrix, ((1,), (0,)))
                for c in range(4):
                    buffer[4 * h + c] = part[:, LANES * c : LANES * (c + 1)]
            for h in range(g.halves):
                for c in range(4):
                    for a in range(4):
                        for b in range(4):
                            pick = pl.ds(4 * g.rows * a + b, g.rows, 4)
                            target[g.row(4 * a + b), g.lane(h, c)] = buffer[4 * h + c, pick, :]

    return body


def first_kernel(g):
    def body(
        xd, sd, m_ref, matrix_ref, r1, r2, r3, r4, rc,
        cx, cxp, cr, crp, cy, inv, z_ref, p1, p2, p3, p4,
        planes, edges, vloc, buffer,
    ):
        even_x, even_r, bottom, top = positions()
        rows = row_index(g)
        lanes = lane_index(g)
        n = 4 * g.rows
        span = LANES * g.halves
        H = range(g.halves)
        matrix = matrix_ref[...]
        for h in H:
            at = pl.ds(g.wide * h, g.wide)
            one, two = r1[0:n, at], r2[0:n, at]
            both = jnp.concatenate([jnp.where(even_x, one, two), jnp.where(even_x, two, one)], 0)
            both = exact_dot(both, matrix, ((1,), (0,)))
            for c in range(4):
                buffer[4 * h + c] = both[:, LANES * c : LANES * (c + 1)]
            for c in range(4):
                for b in range(4):
                    planes[g.row(b), g.lane(h, c)] = buffer[4 * h + c, pl.ds(b, g.rows, 4), :]
                    planes[g.row(4 + b), g.lane(h, c)] = buffer[4 * h + c, pl.ds(n + b, g.rows, 4), :]
        one, two = r3[...], r4[...]
        edges[0:8] = jnp.where(even_r, one, two)
        edges[8:16] = jnp.where(even_r, two, one)
        low_all = edges[12:13, :]
        low = [[jnp.where(bottom, 0.0, low_all[:, span * k + LANES * h : span * k + LANES * (h + 1)]) for h in H] for k in range(3)]
        for h in H:
            at = pl.ds(g.wide * h, g.wide)
            edges[:, at] = exact_dot(edges[:, at], matrix, ((1,), (0,)))
        own = [[m_ref[k, 0, :, g.half(h)] for h in H] for k in range(3)]
        left = []
        for k in range(3):
            pair = []
            for h in H:
                at = pl.ds(span * k + LANES * h, LANES)
                pair.append(jnp.where(even_x, r2[pl.ds(n, g.rows), at], r1[pl.ds(n, g.rows), at]))
            left.append(pair)
        diag_low = [[jnp.where(bottom, 0.0, rc[pl.ds(k, 1), g.half(h)]) for h in H] for k in range(3)]

        def over_y(parts):
            before = prev_lane(parts, lanes)
            return [parts[h] + before[h] for h in H]

        def over_r(parts, edge):
            return [parts[h] + prev_row(parts[h], rows, edge[h]) for h in H]

        def lines_x(parts, edge):
            wide_r = over_r(parts, edge)
            return {(1, 1): parts, (1, 0): over_y(parts), (0, 1): wide_r, (0, 0): over_y(wide_r)}

        for target, table in ((cx, lines_x(own[0], low[0])), (cxp, lines_x(left[0], diag_low[0]))):
            for b in range(4):
                for c in range(4):
                    for h in H:
                        target[g.row(b), g.lane(h, c)] = (W[b] * W[c]) * table[(min(b, 1), min(c, 1))][h]
        zero = [jnp.zeros((g.rows, LANES), F32) for h in H]
        own_r = own[1]
        both_r = [own[1][h] + left[1][h] for h in H]
        table_r = {(1, 1): own_r, (1, 0): over_y(own_r), (0, 1): both_r, (0, 0): over_y(both_r)}
        own_l = [jnp.where(rows == 0, low[1][h], 0.0) for h in H]
        both_l = [jnp.where(rows == 0, low[1][h] + diag_low[1][h], 0.0) for h in H]
        table_l = {(1, 1): own_l, (1, 0): over_y(own_l), (0, 1): both_l, (0, 0): over_y(both_l)}
        for target, table in ((cr, table_r), (crp, table_l)):
            for a in range(4):
                for c in range(4):
                    for h in H:
                        target[g.row(a), g.lane(h, c)] = (W[a] * W[c]) * table[(min(a, 1), min(c, 1))][h]
        both_y = [own[2][h] + left[2][h] for h in H]
        low_y = [low[2][h] + diag_low[2][h] for h in H]
        table_y = {
            (1, 1): own[2],
            (1, 0): over_r(own[2], low[2]),
            (0, 1): both_y,
            (0, 0): over_r(both_y, low_y),
        }
        for a in range(4):
            for b in range(4):
                for h in H:
                    cy[g.row(4 * a + b), g.half(h)] = (W[a] * W[b]) * table_y[(min(a, 1), min(b, 1))][h]
        local_apply(g, xd, cx, cxp, cr, crp, cy, vloc)
        behind = {}
        for key in table_y:
            behind[key] = prev_lane(table_y[key], lanes)
        for h in H:
            for c in range(4):
                at = g.lane(h, c)
                coef_x = [cx[g.row(b), at] for b in range(4)]
                coef_r = [cr[g.row(a), at] for a in range(4)]
                v = [[vloc[g.row(4 * a + b), at] for b in range(4)] for a in range(4)]
                above_x = [planes[g.row(b), at] for b in range(4)]
                below_x = [cxp[g.row(b), at] * planes[g.row(4 + b), at] for b in range(4)]
                above_r = [jnp.where(top, 0.0, edges[pl.ds(a, 1), at]) for a in range(4)]
                below_r = [jnp.where(bottom, 0.0, crp[pl.ds(g.rows * a, 1), at] * edges[pl.ds(8 + a, 1), at]) for a in range(4)]
                add_halo(g, v, coef_x, coef_r, above_x, below_x, above_r, below_r, rows)
                z = [[None] * 4 for _ in range(4)]
                for a in range(4):
                    for b in range(4):
                        weight = W[a] * W[b]
                        key = (min(a, 1), min(b, 1))
                        diag = K[a][a] * coef_x[b] + K[b][b] * coef_r[a]
                        diag = diag + (K[c][c] * weight) * table_y[key][h]
                        if a == 0:
                            diag = diag + K[4][4] * cxp[g.row(b), at]
                        if b == 0:
                            diag = diag + K[4][4] * prev_row(coef_r[a], rows, crp[pl.ds(g.rows * a, 1), at])
                        if c == 0:
                            diag = diag + (K[4][4] * weight) * behind[key][h]
                        scale = 1.0 / diag
                        r = sd[g.row(4 * a + b), at] - v[a][b]
                        z[a][b] = scale * r
                        inv[g.row(4 * a + b), at] = scale
                        z_ref[g.row(4 * a + b), at] = z[a][b]
                send_planes(g, z, at, h, c, coef_x, coef_r, even_x, even_r, (p1, p2, p3, p4))

    return body


def restore(g, sources, targets, matrix, buffer):
    for source, target in zip(sources, targets):
        for h in range(g.halves):
            for c in range(4):
                for a in range(4):
                    for b in range(4):
                        pick = pl.ds(4 * g.rows * a + b, g.rows, 4)
                        buffer[4 * h + c, pick, :] = source[g.row(4 * a + b), g.lane(h, c)]
        for h in range(g.halves):
            part = jnp.concatenate([buffer[4 * h + c] for c in range(4)], 1)
            part = exact_dot(part, matrix, ((1,), (1,)))
            target[:, pl.ds(g.wide * h, g.wide)] = part


def inner_kernel(g, count, with_diagonal):
    def body(*refs):
        cx, cxp, cr, crp, cy, inv, matrix = refs[:7]
        many = refs[7 : 7 + count]
        v_ref, dots, z_plain = refs[7 + count : 10 + count]
        buffer = refs[-1]
        newest = many[-1]
        local_apply(g, newest, cx, cxp, cr, crp, cy, v_ref)
        totals = [jnp.zeros((g.rows, LANES), F32)] * count
        diagonal = refs[-2] if with_diagonal else None
        for ab in range(16):
            for h in range(g.halves):
                for c in range(4):
                    at = (g.row(ab), g.lane(h, c))
                    diag = 1.0 / inv[at]
                    if with_diagonal:
                        diagonal[at] = diag
                    weighted = diag * newest[at]
                    totals = [total + weighted * ref[at] for total, ref in zip(totals, many)]
        for i in range(count):
            dots[pl.ds(g.rows * i, g.rows), :] = totals[i]
        restore(g, [newest], [z_plain], matrix[...], buffer)
        if with_diagonal:
            restore(g, [diagonal], [refs[10 + count]], matrix[...], buffer)

    return body


def received(g, r1, r2, r3, r4, h, c, at, even_x, even_r, bottom, top):
    above_x, below_x, above_r, below_r = [], [], [], []
    for b in range(4):
        one, two = r1[g.row(b), at], r2[g.row(b), at]
        above_x.append(jnp.where(even_x, one, two))
        below_x.append(jnp.where(even_x, two, one))
    for a in range(4):
        one, two = r3[pl.ds(4 * a + c, 1), g.half(h)], r4[pl.ds(4 * a + c, 1), g.half(h)]
        above_r.append(jnp.where(top, 0.0, jnp.where(even_r, one, two)))
        below_r.append(jnp.where(bottom, 0.0, jnp.where(even_r, two, one)))
    return above_x, below_x, above_r, below_r


def next_kernel(g, pulls):
    def body(*refs):
        vloc, cx, cr, inv, r1, r2, r3, r4 = refs[:8]
        earlier = refs[8 : 8 + len(pulls)]
        z_ref, p1, p2, p3, p4 = refs[8 + len(pulls) :]
        even_x, even_r, bottom, top = positions()
        rows = row_index(g)
        for h in range(g.halves):
            for c in range(4):
                at = g.lane(h, c)
                coef_x = [cx[g.row(b), at] for b in range(4)]
                coef_r = [cr[g.row(a), at] for a in range(4)]
                v = [[vloc[g.row(4 * a + b), at] for b in range(4)] for a in range(4)]
                halo = received(g, r1, r2, r3, r4, h, c, at, even_x, even_r, bottom, top)
                add_halo(g, v, coef_x, coef_r, *halo, rows)
                z = [[None] * 4 for _ in range(4)]
                for a in range(4):
                    for b in range(4):
                        rw = g.row(4 * a + b)
                        value = inv[rw, at] * v[a][b]
                        for ref, pull in zip(earlier, pulls):
                            value = value - pull * ref[rw, at]
                        z[a][b] = value
                        z_ref[rw, at] = value
                send_planes(g, z, at, h, c, coef_x, coef_r, even_x, even_r, (p1, p2, p3, p4))

    return body


def last_kernel(g, devices):
    def body(vloc, cx, cr, z_ref, r1, r2, r3, r4, d0, d1, d2, v_ref, message):
        even_x, even_r, bottom, top = positions()
        rows = row_index(g)
        total = jnp.zeros((g.rows, LANES), F32)
        for h in range(g.halves):
            for c in range(4):
                at = g.lane(h, c)
                coef_x = [cx[g.row(b), at] for b in range(4)]
                coef_r = [cr[g.row(a), at] for a in range(4)]
                v = [[vloc[g.row(4 * a + b), at] for b in range(4)] for a in range(4)]
                halo = received(g, r1, r2, r3, r4, h, c, at, even_x, even_r, bottom, top)
                add_halo(g, v, coef_x, coef_r, *halo, rows)
                for a in range(4):
                    for b in range(4):
                        rw = g.row(4 * a + b)
                        v_ref[rw, at] = v[a][b]
                        total = total + z_ref[rw, at] * v[a][b]
        parts = []
        for ref in (d0, d1, d2):
            for i in range(ref.shape[0] // g.rows):
                parts.append(ref[pl.ds(g.rows * i, g.rows), :])
        parts.append(total)
        place = lax.broadcasted_iota(jnp.int32, (g.rows, LANES), 1)
        out = jnp.zeros((g.rows, LANES), F32)
        for i, part in enumerate(parts):
            out = out + jnp.where(place == i, jnp.sum(part, axis=1, keepdims=True), 0.0)
        row = jnp.sum(out, axis=0, keepdims=True)
        message[...] = jnp.broadcast_to(row, (devices, LANES))

    return body


def restore_kernel(g):
    def body(source, x_hbm, target, x_ref, buffer, sems):
        loads = [pltpu.make_async_copy(x_hbm.at[a], x_ref.at[a], sems.at[a]) for a in range(4)]
        for load in loads:
            load.start()
        restore(g, [source], [target], permutation(), buffer)
        for load in loads:
            load.wait()

    return body


def finish_kernel(g):
    def body(sums, x_ref, diag, z0, z1, z2, v3, solution_hbm, residual_hbm, solution_ref, residual_ref, sems):
        total = jnp.sum(sums[...], axis=0, keepdims=True)
        place = lax.broadcasted_iota(jnp.int32, (1, LANES), 1)
        dot = [jnp.sum(jnp.where(place == i, total, 0.0), axis=1, keepdims=True) for i in range(DOTS)]
        s00, s01, s11, s12, s22, m22 = dot
        m00 = s01 + SHIFT * s00
        m01 = s11 + SHIFT * s01
        m02 = s12 + SHIFT * s11
        m11 = m02
        m12 = s22 + SHIFT * s12
        l10 = m01 / m00
        l20 = m02 / m00
        d1 = m11 - l10 * m01
        t = m12 - l10 * m02
        l21 = t / d1
        d2 = m22 - l20 * m02 - l21 * t
        y1 = s01 - l10 * s00
        y2 = s11 - l20 * s00 - l21 * y1
        c2 = y2 / d2
        c1 = y1 / d1 - l21 * c2
        c0 = s00 / m00 - l10 * c1 - l20 * c2
        e0 = 1.0 - SHIFT * c0
        e1 = c0 + SHIFT * c1
        copies = []
        for a in range(4):
            at = pl.ds(4 * g.rows * a, 4 * g.rows)
            p0, p1, p2 = z0[at], z1[at], z2[at]
            residual_ref[a] = diag[at] * (e0 * p0 - (e1 * p1 + c1 * p2)) - c2 * v3[at]
            copies.append(pltpu.make_async_copy(residual_ref.at[a], residual_hbm.at[a], sems.at[4 + a]))
            copies[-1].start()
            solution_ref[a] = x_ref[a] + (c0 * p0 + (c1 * p1 + c2 * p2))
            copies.append(pltpu.make_async_copy(solution_ref.at[a], solution_hbm.at[a], sems.at[a]))
            copies[-1].start()
        for copy in copies:
            copy.wait()

    return body


def swaps(count, parity):
    pairs = []
    for i in range(count):
        step = 1 if i % 2 == parity else -1
        pairs.append((i, (i + step) % count))
    return pairs


VMEM = pl.BlockSpec(memory_space=pltpu.VMEM)
HBM = pl.BlockSpec(memory_space=pltpu.HBM)
MIB = 1024 * 1024


def call(body, args, outs, scratch=(), limit=6, in_specs=None, out_specs=None, aliases=None, flops=1000000):
    return pl.pallas_call(
        body,
        in_specs=in_specs or [VMEM] * len(args),
        out_specs=out_specs or [VMEM] * len(outs),
        out_shape=[jax.ShapeDtypeStruct(s, t) for s, t in outs],
        scratch_shapes=list(scratch),
        input_output_aliases=aliases or {},
        cost_estimate=pl.CostEstimate(flops=flops, bytes_accessed=1000000, transcendentals=0),
        compiler_params=pltpu.CompilerParams(vmem_limit_bytes=limit * MIB),
    )(*args)


def steps(source_term, initial_guess, metric):
    count_x, count_r, count_y = metric.shape[1:]
    assert count_x == 1 and count_r == ROWS and count_y % LANES == 0
    g = Shape(count_r, count_y)
    nx, nr = lax.axis_size("group"), lax.axis_size("rad")
    assert nx % 2 == 0 and nr % 2 == 0
    full = ((16 * count_r, 4 * count_y), F32)
    plane = ((4 * count_r, 4 * count_y), F32)
    edge = ((16, count_y), F32)
    natural = (initial_guess.shape, F32)

    def exchange(p1, p2, p3, p4):
        sends = ((p1, "group", nx, 0), (p2, "group", nx, 1), (p3, "rad", nr, 0), (p4, "rad", nr, 1))
        got = []
        for value, axis, count, parity in sends:
            got.append(lax.ppermute(value, axis, swaps(count, parity)))
        return tuple(got)

    guess = pltpu.with_memory_space_constraint(initial_guess, pltpu.HBM)
    x0, m0, p1, p2, p3, p4, corner = call(
        start_kernel(g),
        (guess, pltpu.with_memory_space_constraint(metric, pltpu.HBM)),
        [natural, (metric.shape, F32)]
        + [((5 * count_r, 4 * count_y), F32)] * 2 + [((8, 4 * count_y), F32)] * 2 + [((8, count_y), F32)],
        [pltpu.SemaphoreType.DMA((5,))],
        in_specs=[HBM, HBM],
    )
    got = exchange(p1, p2, p3, p4)
    diagonal = [
        (i * nr + j, ((i + 1) % nx) * nr + (j + 1) % nr) for i in range(nx) for j in range(nr)
    ]
    corner = lax.ppermute(corner, ("group", "rad"), diagonal)
    matrix = ((4 * LANES, 4 * LANES), BF16)
    tiles = pltpu.VMEM((4 * g.halves, 16 * count_r, LANES), F32)
    xd, sd, matrix = call(
        arrange_kernel(g),
        (x0, source_term),
        [full, full, matrix],
        [tiles],
    )
    outs = [plane, plane, plane, plane, ((16 * count_r, count_y), F32), full, full]
    outs += [plane, plane, edge, edge]
    cx, cxp, cr, crp, cy, inv, z0, *send = call(
        first_kernel(g),
        (xd, sd, m0, matrix, *got, corner),
        outs,
        [pltpu.VMEM((8 * count_r, 4 * count_y), F32), pltpu.VMEM((16, 4 * count_y), F32), pltpu.VMEM(*full), pltpu.VMEM((count_y // 32, 8 * count_r, LANES), F32)],
    )

    def inner(many, with_diagonal):
        return call(
            inner_kernel(g, len(many), with_diagonal),
            (cx, cxp, cr, crp, cy, inv, matrix, *many),
            [full, ((count_r * len(many), LANES), F32), full] + [full] * with_diagonal,
            [pltpu.VMEM(*full)] * with_diagonal + [tiles],
        )

    def step(vloc, got, earlier, pulls):
        z, *send = call(
            next_kernel(g, pulls),
            (vloc, cx, cr, inv, *got, *earlier),
            [full, plane, plane, edge, edge],
        )
        return z, send

    got = exchange(*send)
    vloc, d0, z0_n, diag_n = inner((z0,), True)
    z1, send = step(vloc, got, (z0,), (SHIFT,))
    got = exchange(*send)
    vloc, d1, z1_n = inner((z0, z1), False)
    z2, send = step(vloc, got, (z1,), (SHIFT,))
    got = exchange(*send)
    vloc, d2, z2_n = inner((z1, z2), False)
    v3, message = call(
        last_kernel(g, nx * nr),
        (vloc, cx, cr, z2, *got, d0, d1, d2),
        [full, ((nx * nr, LANES), F32)],
    )
    sums = lax.all_to_all(message, ("group", "rad"), 0, 0, tiled=True)
    v3_n, x0 = call(
        restore_kernel(g),
        (v3, guess),
        [full, natural],
        [tiles, pltpu.SemaphoreType.DMA((4,))],
        in_specs=[VMEM, HBM],
        aliases={0: 0},
    )
    return tuple(
        call(
            finish_kernel(g),
            (sums, x0, diag_n, z0_n, z1_n, z2_n, v3_n),
            [natural, natural],
            [pltpu.VMEM(*natural)] * 2 + [pltpu.SemaphoreType.DMA((8,))],
            out_specs=[HBM, HBM],
        )
    )


def solution(mesh):
    in_specs = (P("group", "rad", None), P("group", "rad", None), P(None, "group", "rad", None))
    out_specs = (P("group", "rad", None), P("group", "rad", None))
    return jax.shard_map(steps, mesh=mesh, in_specs=in_specs, out_specs=out_specs, check_vma=False)
```

```python
import math

import jax
import jax.numpy as jnp
import numpy as np
from jax import lax
from jax.experimental import pallas as pl
from jax.experimental.pallas import tpu as pltpu
from jax.sharding import PartitionSpec as P

F32 = jnp.float32
BF16 = jnp.bfloat16
LANES = 128
ROWS = 8
SHIFT = 1.145
DOTS = 5
FOLD = LANES // 2


def gll_tables():
    root = math.sqrt(3.0 / 7.0)
    points = np.array([-1.0, -root, 0.0, root, 1.0])
    weights = np.array([0.1, 49.0 / 90.0, 32.0 / 45.0, 49.0 / 90.0, 0.1])
    factor = np.array(
        [np.prod([points[a] - points[m] for m in range(5) if m != a]) for a in range(5)]
    )
    derivative = np.zeros((5, 5))
    for p in range(5):
        for a in range(5):
            if p == a:
                derivative[p, a] = np.sum(
                    [1.0 / (points[a] - points[m]) for m in range(5) if m != a]
                )
            else:
                derivative[p, a] = factor[p] / (factor[a] * (points[p] - points[a]))
    return derivative, weights


DERIVATIVE, WEIGHTS = gll_tables()
STIFF = DERIVATIVE.T @ np.diag(WEIGHTS) @ DERIVATIVE
K = [[float(v) for v in row] for row in STIFF]
W = [float(v) for v in WEIGHTS]


def line_operator(u):
    u0, u1, u2, u3, u4 = u
    s = u0 if u4 is None else u0 + u4
    o0 = u0 if u4 is None else u0 - u4
    t = u1 + u3
    o1 = u1 - u3
    q = u2 + u2
    d0 = s - q
    d1 = t - q
    e0 = (0.5 * (K[0][0] + K[0][4])) * d0 + (0.5 * (K[0][1] + K[0][3])) * d1
    e1 = (0.5 * (K[1][0] + K[1][4])) * d0 + (0.5 * (K[1][1] + K[1][3])) * d1
    p0 = (0.5 * (K[0][0] - K[0][4])) * o0 + (0.5 * (K[0][1] - K[0][3])) * o1
    p1 = (0.5 * (K[1][0] - K[1][4])) * o0 + (0.5 * (K[1][1] - K[1][3])) * o1
    e = e0 + e1
    return e0 + p0, e1 + p1, -(e + e), e1 - p1, e0 - p0


def last_row(u):
    return K[4][0] * u[0] + K[4][1] * u[1] + K[4][2] * u[2] + K[4][3] * u[3]


class Shape:
    def __init__(self, count_r, count_y):
        self.rows = count_r
        self.halves = count_y // LANES
        self.wide = 4 * LANES

    def row(self, index):
        return pl.ds(self.rows * index, self.rows)

    def lane(self, h, c):
        return pl.ds(self.wide * h + LANES * c, LANES)

    def half(self, h):
        return pl.ds(LANES * h, LANES)


def row_index(g):
    return lax.broadcasted_iota(jnp.int32, (g.rows, LANES), 0)


def lane_index(g):
    return lax.broadcasted_iota(jnp.int32, (g.rows, LANES), 1)


def next_lane(parts, lanes):
    rolled = [pltpu.roll(p, LANES - 1, 1) for p in parts]
    n = len(parts)
    return [jnp.where(lanes == LANES - 1, rolled[(h + 1) % n], rolled[h]) for h in range(n)]


def prev_lane(parts, lanes):
    rolled = [pltpu.roll(p, 1, 1) for p in parts]
    n = len(parts)
    return [jnp.where(lanes == 0, rolled[(h - 1) % n], rolled[h]) for h in range(n)]


def next_row(g, value, rows, last):
    return jnp.where(rows == g.rows - 1, last, pltpu.roll(value, g.rows - 1, 0))


def prev_row(value, rows, first):
    return jnp.where(rows == 0, first, pltpu.roll(value, 1, 0))


def permutation():
    source = lax.broadcasted_iota(jnp.int32, (4 * LANES, 4 * LANES), 0)
    target = lax.broadcasted_iota(jnp.int32, (4 * LANES, 4 * LANES), 1)
    wanted = (target % LANES) * 4 + target // LANES
    return jnp.where(source == wanted, 1.0, 0.0).astype(BF16)


def exact_dot(blocks, matrix, dims):
    parts = []
    for values in blocks:
        one = values.astype(BF16)
        rest = values - one.astype(F32)
        two = rest.astype(BF16)
        three = (rest - two.astype(F32)).astype(BF16)
        parts += [one, two, three]
    product = lax.dot_general(
        jnp.concatenate(parts, 0), matrix, (dims, ((), ())), preferred_element_type=F32
    )
    out = []
    first = 0
    for values in blocks:
        n = values.shape[0]
        one, two, three = (product[first + n * i : first + n * (i + 1)] for i in range(3))
        out.append((one + two) + three)
        first += 3 * n
    return out


def local_apply(g, u_ref, cx, cxp, cr, crp, cy, v_ref):
    rows = row_index(g)
    lanes = lane_index(g)
    for ab in range(16):
        u = [[u_ref[g.row(ab), g.lane(h, c)] for c in range(4)] for h in range(g.halves)]
        fifth = next_lane([u[h][0] for h in range(g.halves)], lanes)
        ends = []
        outs = []
        for h in range(g.halves):
            coef = cy[g.row(ab), g.half(h)]
            r = line_operator(u[h] + [fifth[h]])
            outs.append([coef * r[c] for c in range(4)])
            ends.append(coef * r[4])
        ends = prev_lane(ends, lanes)
        for h in range(g.halves):
            outs[h][0] = outs[h][0] + ends[h]
            for c in range(4):
                v_ref[g.row(ab), g.lane(h, c)] = outs[h][c]
    for h in range(g.halves):
        for c in range(4):
            at = g.lane(h, c)
            u = [[u_ref[g.row(4 * a + b), at] for b in range(4)] for a in range(4)]
            v = [[v_ref[g.row(4 * a + b), at] for b in range(4)] for a in range(4)]
            for b in range(4):
                coef = cx[g.row(b), at]
                r = line_operator([u[a][b] for a in range(4)] + [None])
                for a in range(4):
                    v[a][b] = v[a][b] + coef * r[a]
                v[0][b] = v[0][b] + K[4][4] * (cxp[g.row(b), at] * u[0][b])
            for a in range(4):
                coef = cr[g.row(a), at]
                r = line_operator(u[a] + [next_row(g, u[a][0], rows, 0.0)])
                for b in range(4):
                    v[a][b] = v[a][b] + coef * r[b]
                v[a][0] = v[a][0] + prev_row(coef * r[4], rows, 0.0)
                v[a][0] = v[a][0] + K[4][4] * (crp[g.row(a), at] * u[a][0])
            for a in range(4):
                for b in range(4):
                    v_ref[g.row(4 * a + b), at] = v[a][b]


def add_halo(g, v, coef_x, coef_r, above_x, below_x, above_r, below_r, rows):
    for b in range(4):
        reach = coef_x[b] * above_x[b]
        for a in range(4):
            v[a][b] = v[a][b] + K[a][4] * reach
        v[0][b] = v[0][b] + below_x[b]
    for a in range(4):
        reach = jnp.where(rows == g.rows - 1, coef_r[a] * above_r[a], 0.0)
        for b in range(4):
            v[a][b] = v[a][b] + K[b][4] * reach
        v[a][0] = v[a][0] + jnp.where(rows == 0, below_r[a], 0.0)


def send_planes(g, z, at, h, c, coef_x, coef_r, even_x, even_r, out):
    p1, p2, p3, p4 = out
    for b in range(4):
        down = z[0][b]
        up = coef_x[b] * last_row([z[a][b] for a in range(4)])
        p1[g.row(b), at] = jnp.where(even_x, up, down)
        p2[g.row(b), at] = jnp.where(even_x, down, up)
    for a in range(4):
        down = z[a][0][0:1]
        up = (coef_r[a] * last_row(z[a]))[g.rows - 1 :]
        p3[pl.ds(4 * a + c, 1), g.half(h)] = jnp.where(even_r, up, down)
        p4[pl.ds(4 * a + c, 1), g.half(h)] = jnp.where(even_r, down, up)


def positions():
    ix = lax.axis_index("group")
    ir = lax.axis_index("rad")
    top = ir == lax.axis_size("rad") - 1
    return ix % 2 == 0, ir % 2 == 0, ir == 0, top


def start_kernel(g):
    def body(x_hbm, m_hbm, x_ref, m_ref, p1, p2, p3, p4, corner, sems):
        cut = [(a, g.row(b)) for b in range(4) for a in range(4)]
        copies = [pltpu.make_async_copy(x_hbm.at[at], x_ref.at[at], sems.at[i]) for i, at in enumerate(cut)]
        copies.append(pltpu.make_async_copy(m_hbm, m_ref, sems.at[16]))
        for copy in copies:
            copy.start()
        even_x, even_r, _, _ = positions()
        last = g.rows - 1
        n = 4 * g.rows
        span = LANES * g.halves
        corner[...] = jnp.zeros_like(corner)
        p3[...] = jnp.zeros_like(p3)
        p4[...] = jnp.zeros_like(p4)
        for b in range(4):
            at = g.row(b)
            for copy in copies[4 * b : 4 * b + 4]:
                copy.wait()
            down = x_ref[0, at]
            up = last_row([x_ref[a, at] for a in range(4)])
            p1[at] = jnp.where(even_x, up, down)
            p2[at] = jnp.where(even_x, down, up)
        copies[-1].wait()
        for k in range(3):
            m = m_ref[k, 0]
            p1[pl.ds(n, g.rows), pl.ds(span * k, span)] = m
            p2[pl.ds(n, g.rows), pl.ds(span * k, span)] = m
            edge = m[last:]
            corner[pl.ds(k, 1), :] = edge
            p3[pl.ds(4, 1), pl.ds(span * k, span)] = edge
            p4[pl.ds(4, 1), pl.ds(span * k, span)] = edge
        p1[pl.ds(n, g.rows), pl.ds(span * 3, span)] = m
        p2[pl.ds(n, g.rows), pl.ds(span * 3, span)] = m
        for a in range(4):
            down = x_ref[a, 0:1]
            up = last_row([x_ref[a, pl.ds(4 * last + b, 1)] for b in range(4)])
            p3[pl.ds(a, 1)] = jnp.where(even_r, up, down)
            p4[pl.ds(a, 1)] = jnp.where(even_r, down, up)

    return body


def line_results(g, u_ref, along_x, along_r, end_r, along_y, end_y):
    rows = row_index(g)
    lanes = lane_index(g)
    for ab in range(16):
        u = [[u_ref[g.row(ab), g.lane(h, c)] for c in range(4)] for h in range(g.halves)]
        fifth = next_lane([u[h][0] for h in range(g.halves)], lanes)
        for h in range(g.halves):
            r = line_operator(u[h] + [fifth[h]])
            for c in range(4):
                along_y[g.row(ab), g.lane(h, c)] = r[c]
            end_y[g.row(ab), g.half(h)] = r[4]
    for h in range(g.halves):
        for c in range(4):
            at = g.lane(h, c)
            u = [[u_ref[g.row(4 * a + b), at] for b in range(4)] for a in range(4)]
            for b in range(4):
                r = line_operator([u[a][b] for a in range(4)] + [None])
                for a in range(4):
                    along_x[g.row(4 * a + b), at] = r[a]
            for a in range(4):
                r = line_operator(u[a] + [next_row(g, u[a][0], rows, 0.0)])
                for b in range(4):
                    along_r[g.row(4 * a + b), at] = r[b]
                end_r[g.row(a), at] = r[4]


def arrange_kernel(g):
    def body(x_ref, s_ref, xd, sd, matrix_ref, along_x, along_r, end_r, along_y, end_y, buffer):
        matrix = permutation()
        matrix_ref[...] = matrix
        for source, target in ((x_ref, xd), (s_ref, sd)):
            blocks = [
                source[:, :, pl.ds(g.wide * h, g.wide)].reshape(16 * g.rows, g.wide) for h in range(g.halves)
            ]
            blocks = exact_dot(blocks, matrix, ((1,), (0,)))
            for h in range(g.halves):
                for c in range(4):
                    buffer[4 * h + c] = blocks[h][:, LANES * c : LANES * (c + 1)]
            for h in range(g.halves):
                for c in range(4):
                    for a in range(4):
                        for b in range(4):
                            pick = pl.ds(4 * g.rows * a + b, g.rows, 4)
                            target[g.row(4 * a + b), g.lane(h, c)] = buffer[4 * h + c, pick, :]
        line_results(g, xd, along_x, along_r, end_r, along_y, end_y)

    return body


def first_kernel(g):
    def body(
        xd, sd, along_x, along_r, end_r, along_y, end_y, m_ref, matrix_ref, r1, r2, r3, r4, rc,
        cx, cxp, cr, crp, cy, inv, z_ref, p1, p2, p3, p4,
        planes, edges, buffer,
    ):
        even_x, even_r, bottom, top = positions()
        rows = row_index(g)
        lanes = lane_index(g)
        n = 4 * g.rows
        span = LANES * g.halves
        H = range(g.halves)
        matrix = matrix_ref[...]
        low_all = jnp.where(even_r, r4[4:5, :], r3[4:5, :])
        blocks = []
        for h in H:
            at = pl.ds(g.wide * h, g.wide)
            one, two = r1[0:n, at], r2[0:n, at]
            blocks += [jnp.where(even_x, one, two), jnp.where(even_x, two, one)]
            one, two = r3[:, at], r4[:, at]
            blocks += [jnp.where(even_r, one, two), jnp.where(even_r, two, one)]
        blocks = exact_dot(blocks, matrix, ((1,), (0,)))
        for h in H:
            for c in range(4):
                lanes_c = slice(LANES * c, LANES * (c + 1))
                buffer[4 * h + c, 0:n] = blocks[4 * h][:, lanes_c]
                buffer[4 * h + c, n : 2 * n] = blocks[4 * h + 1][:, lanes_c]
                edges[0:8, g.lane(h, c)] = blocks[4 * h + 2][:, lanes_c]
                edges[8:16, g.lane(h, c)] = blocks[4 * h + 3][:, lanes_c]
            for c in range(4):
                for b in range(4):
                    planes[g.row(b), g.lane(h, c)] = buffer[4 * h + c, pl.ds(b, g.rows, 4), :]
                    planes[g.row(4 + b), g.lane(h, c)] = buffer[4 * h + c, pl.ds(n + b, g.rows, 4), :]
        low = [[jnp.where(bottom, 0.0, low_all[:, span * k + LANES * h : span * k + LANES * (h + 1)]) for h in H] for k in range(3)]
        own = [[m_ref[k, 0, :, g.half(h)] for h in H] for k in range(3)]
        left = []
        for k in range(3):
            pair = []
            for h in H:
                at = pl.ds(span * k + LANES * h, LANES)
                pair.append(jnp.where(even_x, r2[pl.ds(n, g.rows), at], r1[pl.ds(n, g.rows), at]))
            left.append(pair)
        diag_low = [[jnp.where(bottom, 0.0, rc[pl.ds(k, 1), g.half(h)]) for h in H] for k in range(3)]

        def over_y(parts):
            before = prev_lane(parts, lanes)
            return [parts[h] + before[h] for h in H]

        def over_r(parts, edge):
            return [parts[h] + prev_row(parts[h], rows, edge[h]) for h in H]

        def lines_x(parts, edge):
            wide_r = over_r(parts, edge)
            return {(1, 1): parts, (1, 0): over_y(parts), (0, 1): wide_r, (0, 0): over_y(wide_r)}

        for target, table in ((cx, lines_x(own[0], low[0])), (cxp, lines_x(left[0], diag_low[0]))):
            for b in range(4):
                for c in range(4):
                    for h in H:
                        target[g.row(b), g.lane(h, c)] = (W[b] * W[c]) * table[(min(b, 1), min(c, 1))][h]
        zero = [jnp.zeros((g.rows, LANES), F32) for h in H]
        own_r = own[1]
        both_r = [own[1][h] + left[1][h] for h in H]
        table_r = {(1, 1): own_r, (1, 0): over_y(own_r), (0, 1): both_r, (0, 0): over_y(both_r)}
        own_l = [jnp.where(rows == 0, low[1][h], 0.0) for h in H]
        both_l = [jnp.where(rows == 0, low[1][h] + diag_low[1][h], 0.0) for h in H]
        table_l = {(1, 1): own_l, (1, 0): over_y(own_l), (0, 1): both_l, (0, 0): over_y(both_l)}
        for target, table in ((cr, table_r), (crp, table_l)):
            for a in range(4):
                for c in range(4):
                    for h in H:
                        target[g.row(a), g.lane(h, c)] = (W[a] * W[c]) * table[(min(a, 1), min(c, 1))][h]
        both_y = [own[2][h] + left[2][h] for h in H]
        low_y = [low[2][h] + diag_low[2][h] for h in H]
        table_y = {
            (1, 1): own[2],
            (1, 0): over_r(own[2], low[2]),
            (0, 1): both_y,
            (0, 0): over_r(both_y, low_y),
        }
        for a in range(4):
            for b in range(4):
                for h in H:
                    cy[g.row(4 * a + b), g.half(h)] = (W[a] * W[b]) * table_y[(min(a, 1), min(b, 1))][h]
        behind = {}
        for key in table_y:
            behind[key] = prev_lane(table_y[key], lanes)
        for h in H:
            for c in range(4):
                at = g.lane(h, c)
                coef_x = [cx[g.row(b), at] for b in range(4)]
                coef_r = [cr[g.row(a), at] for a in range(4)]
                u = [[xd[g.row(4 * a + b), at] for b in range(4)] for a in range(4)]
                v = [[None] * 4 for _ in range(4)]
                for a in range(4):
                    for b in range(4):
                        rw = g.row(4 * a + b)
                        v[a][b] = coef_x[b] * along_x[rw, at] + coef_r[a] * along_r[rw, at]
                        v[a][b] = v[a][b] + cy[rw, g.half(h)] * along_y[rw, at]
                        if c == 0:
                            ends = [cy[rw, g.half(k)] * end_y[rw, g.half(k)] for k in H]
                            v[a][b] = v[a][b] + prev_lane(ends, lanes)[h]
                    v[a][0] = v[a][0] + prev_row(coef_r[a] * end_r[g.row(a), at], rows, 0.0)
                    v[a][0] = v[a][0] + K[4][4] * (crp[g.row(a), at] * u[a][0])
                for b in range(4):
                    v[0][b] = v[0][b] + K[4][4] * (cxp[g.row(b), at] * u[0][b])
                above_x = [planes[g.row(b), at] for b in range(4)]
                below_x = [cxp[g.row(b), at] * planes[g.row(4 + b), at] for b in range(4)]
                above_r = [jnp.where(top, 0.0, edges[pl.ds(a, 1), at]) for a in range(4)]
                below_r = [jnp.where(bottom, 0.0, crp[pl.ds(g.rows * a, 1), at] * edges[pl.ds(8 + a, 1), at]) for a in range(4)]
                add_halo(g, v, coef_x, coef_r, above_x, below_x, above_r, below_r, rows)
                z = [[None] * 4 for _ in range(4)]
                for a in range(4):
                    for b in range(4):
                        weight = W[a] * W[b]
                        key = (min(a, 1), min(b, 1))
                        diag = K[a][a] * coef_x[b] + K[b][b] * coef_r[a]
                        diag = diag + (K[c][c] * weight) * table_y[key][h]
                        if a == 0:
                            diag = diag + K[4][4] * cxp[g.row(b), at]
                        if b == 0:
                            diag = diag + K[4][4] * prev_row(coef_r[a], rows, crp[pl.ds(g.rows * a, 1), at])
                        if c == 0:
                            diag = diag + (K[4][4] * weight) * behind[key][h]
                        scale = 1.0 / diag
                        r = sd[g.row(4 * a + b), at] - v[a][b]
                        z[a][b] = scale * r
                        inv[g.row(4 * a + b), at] = scale
                        z_ref[g.row(4 * a + b), at] = z[a][b]
                send_planes(g, z, at, h, c, coef_x, coef_r, even_x, even_r, (p1, p2, p3, p4))

    return body


def restore(g, sources, targets, matrix, buffer):
    for source, target in zip(sources, targets):
        for h in range(g.halves):
            for c in range(4):
                for a in range(4):
                    for b in range(4):
                        pick = pl.ds(4 * g.rows * a + b, g.rows, 4)
                        buffer[4 * h + c, pick, :] = source[g.row(4 * a + b), g.lane(h, c)]
        blocks = [jnp.concatenate([buffer[4 * h + c] for c in range(4)], 1) for h in range(g.halves)]
        blocks = exact_dot(blocks, matrix, ((1,), (1,)))
        for h in range(g.halves):
            target[:, pl.ds(g.wide * h, g.wide)] = blocks[h]


def inner_kernel(g, count, with_diagonal, earlier):
    def body(*refs):
        cx, cxp, cr, crp, cy, inv, matrix = refs[:7]
        many = refs[7 : 7 + count]
        before = refs[7 + count : 7 + count + earlier]
        refs = refs[:7] + many + refs[7 + count + earlier :]
        v_ref, dots, z_plain = refs[7 + count : 10 + count]
        buffer = refs[-1]
        newest = many[-1]
        local_apply(g, newest, cx, cxp, cr, crp, cy, v_ref)
        totals = [jnp.zeros((g.rows, LANES), F32)] * count
        diagonal = refs[-2] if with_diagonal else None
        for ab in range(16):
            for h in range(g.halves):
                for c in range(4):
                    at = (g.row(ab), g.lane(h, c))
                    diag = 1.0 / inv[at]
                    if with_diagonal:
                        diagonal[at] = diag
                    weighted = diag * newest[at]
                    totals = [total + weighted * ref[at] for total, ref in zip(totals, many)]
        if earlier:
            parts = [ref[pl.ds(i, g.rows), :] for ref in before for i in range(0, ref.shape[0], g.rows)]
            place = lane_index(g)
            row = jnp.zeros((g.rows, LANES), F32)
            for i, part in enumerate(parts + totals):
                row = row + jnp.where(place == FOLD + i, jnp.sum(part, axis=1, keepdims=True), 0.0)
            dots[...] = jnp.broadcast_to(jnp.sum(row, axis=0, keepdims=True), (g.rows, LANES))
        else:
            for i in range(count):
                dots[pl.ds(g.rows * i, g.rows), :] = totals[i]
        restore(g, [newest], [z_plain], matrix[...], buffer)
        if with_diagonal:
            restore(g, [diagonal], [refs[10 + count]], matrix[...], buffer)

    return body


def received(g, r1, r2, r3, r4, h, c, at, even_x, even_r, bottom, top):
    above_x, below_x, above_r, below_r = [], [], [], []
    for b in range(4):
        one, two = r1[g.row(b), at], r2[g.row(b), at]
        above_x.append(jnp.where(even_x, one, two))
        below_x.append(jnp.where(even_x, two, one))
    for a in range(4):
        one, two = r3[pl.ds(4 * a + c, 1), g.half(h)], r4[pl.ds(4 * a + c, 1), g.half(h)]
        above_r.append(jnp.where(top, 0.0, jnp.where(even_r, one, two)))
        below_r.append(jnp.where(bottom, 0.0, jnp.where(even_r, two, one)))
    return above_x, below_x, above_r, below_r


def next_kernel(g, pulls):
    def body(*refs):
        vloc, cx, cr, inv, r1, r2, r3, r4 = refs[:8]
        earlier = refs[8 : 8 + len(pulls)]
        z_ref, p1, p2, p3, p4 = refs[8 + len(pulls) :]
        even_x, even_r, bottom, top = positions()
        rows = row_index(g)
        for h in range(g.halves):
            for c in range(4):
                at = g.lane(h, c)
                coef_x = [cx[g.row(b), at] for b in range(4)]
                coef_r = [cr[g.row(a), at] for a in range(4)]
                v = [[vloc[g.row(4 * a + b), at] for b in range(4)] for a in range(4)]
                halo = received(g, r1, r2, r3, r4, h, c, at, even_x, even_r, bottom, top)
                add_halo(g, v, coef_x, coef_r, *halo, rows)
                z = [[None] * 4 for _ in range(4)]
                for a in range(4):
                    for b in range(4):
                        rw = g.row(4 * a + b)
                        value = inv[rw, at] * v[a][b]
                        for ref, pull in zip(earlier, pulls):
                            value = value - pull * ref[rw, at]
                        z[a][b] = value
                        z_ref[rw, at] = value
                send_planes(g, z, at, h, c, coef_x, coef_r, even_x, even_r, (p1, p2, p3, p4))

    return body


def last_kernel(g, devices):
    def body(vloc, cx, cr, z_ref, r1, r2, r3, r4, dots, v_ref, message):
        even_x, even_r, bottom, top = positions()
        rows = row_index(g)
        totals = []
        for h in range(g.halves):
            for c in range(4):
                at = g.lane(h, c)
                coef_x = [cx[g.row(b), at] for b in range(4)]
                coef_r = [cr[g.row(a), at] for a in range(4)]
                v = [[vloc[g.row(4 * a + b), at] for b in range(4)] for a in range(4)]
                halo = received(g, r1, r2, r3, r4, h, c, at, even_x, even_r, bottom, top)
                add_halo(g, v, coef_x, coef_r, *halo, rows)
                for a in range(4):
                    total = jnp.zeros((g.rows, LANES), F32)
                    for b in range(4):
                        rw = g.row(4 * a + b)
                        v_ref[rw, at] = v[a][b]
                        total = total + z_ref[rw, at] * v[a][b]
                    totals.append(total)
        while len(totals) > 1:
            totals = [sum(totals[i : i + 2]) for i in range(0, len(totals), 2)]
        row = jnp.sum(totals[0], axis=0, keepdims=True)
        row = row + pltpu.roll(row, FOLD, 1)
        place = lax.broadcasted_iota(jnp.int32, (1, LANES), 1)
        row = jnp.where(place < FOLD, row, dots[0:1])
        message[...] = jnp.broadcast_to(row, (devices, LANES))

    return body


def restore_kernel(g):
    def body(source, x_hbm, target, x_ref, buffer, sems):
        loads = [pltpu.make_async_copy(x_hbm.at[a], x_ref.at[a], sems.at[a]) for a in range(4)]
        for load in loads:
            load.start()
        restore(g, [source], [target], permutation(), buffer)
        for load in loads:
            load.wait()

    return body


def finish_kernel(g):
    def body(sums, x_ref, diag, z0, z1, z2, v3, solution_hbm, residual_hbm, solution_ref, residual_ref, sems):
        total = jnp.sum(sums[...], axis=0, keepdims=True)
        place = lax.broadcasted_iota(jnp.int32, (1, LANES), 1)
        picks = [place == FOLD + i for i in range(DOTS)] + [place < FOLD]
        dot = [jnp.sum(jnp.where(pick, total, 0.0), axis=1, keepdims=True) for pick in picks]
        s00, s01, s11, s12, s22, m22 = dot
        m00 = s01 + SHIFT * s00
        m01 = s11 + SHIFT * s01
        m02 = s12 + SHIFT * s11
        m11 = m02
        m12 = s22 + SHIFT * s12
        l10 = m01 / m00
        l20 = m02 / m00
        d1 = m11 - l10 * m01
        t = m12 - l10 * m02
        l21 = t / d1
        d2 = m22 - l20 * m02 - l21 * t
        y1 = s01 - l10 * s00
        y2 = s11 - l20 * s00 - l21 * y1
        c2 = y2 / d2
        c1 = y1 / d1 - l21 * c2
        c0 = s00 / m00 - l10 * c1 - l20 * c2
        e0 = 1.0 - SHIFT * c0
        e1 = c0 + SHIFT * c1
        copies = []
        for a in range(4):
            at = pl.ds(4 * g.rows * a, 4 * g.rows)
            p0, p1, p2 = z0[at], z1[at], z2[at]
            residual_ref[a] = diag[at] * (e0 * p0 - (e1 * p1 + c1 * p2)) - c2 * v3[at]
            copies.append(pltpu.make_async_copy(residual_ref.at[a], residual_hbm.at[a], sems.at[4 + a]))
            copies[-1].start()
            solution_ref[a] = x_ref[a] + (c0 * p0 + (c1 * p1 + c2 * p2))
            copies.append(pltpu.make_async_copy(solution_ref.at[a], solution_hbm.at[a], sems.at[a]))
            copies[-1].start()
        for copy in copies:
            copy.wait()

    return body


def swaps(count, parity):
    pairs = []
    for i in range(count):
        step = 1 if i % 2 == parity else -1
        pairs.append((i, (i + step) % count))
    return pairs


VMEM = pl.BlockSpec(memory_space=pltpu.VMEM)
HBM = pl.BlockSpec(memory_space=pltpu.HBM)
MIB = 1024 * 1024


def call(body, args, outs, scratch=(), limit=6, in_specs=None, out_specs=None, aliases=None, flops=1000000):
    return pl.pallas_call(
        body,
        in_specs=in_specs or [VMEM] * len(args),
        out_specs=out_specs or [VMEM] * len(outs),
        out_shape=[jax.ShapeDtypeStruct(s, t) for s, t in outs],
        scratch_shapes=list(scratch),
        input_output_aliases=aliases or {},
        cost_estimate=pl.CostEstimate(flops=flops, bytes_accessed=1000000, transcendentals=0),
        compiler_params=pltpu.CompilerParams(vmem_limit_bytes=limit * MIB),
    )(*args)


def steps(source_term, initial_guess, metric):
    count_x, count_r, count_y = metric.shape[1:]
    assert count_x == 1 and count_r == ROWS and count_y % LANES == 0
    g = Shape(count_r, count_y)
    nx, nr = lax.axis_size("group"), lax.axis_size("rad")
    assert nx % 2 == 0 and nr % 2 == 0
    full = ((16 * count_r, 4 * count_y), F32)
    plane = ((4 * count_r, 4 * count_y), F32)
    edge = ((16, count_y), F32)
    natural = (initial_guess.shape, F32)

    def exchange(p1, p2, p3, p4):
        sends = ((p1, "group", nx, 0), (p2, "group", nx, 1), (p3, "rad", nr, 0), (p4, "rad", nr, 1))
        got = []
        for value, axis, count, parity in sends:
            got.append(lax.ppermute(value, axis, swaps(count, parity)))
        return tuple(got)

    guess = pltpu.with_memory_space_constraint(initial_guess, pltpu.HBM)
    x0, m0, p1, p2, p3, p4, corner = call(
        start_kernel(g),
        (guess, pltpu.with_memory_space_constraint(metric, pltpu.HBM)),
        [natural, (metric.shape, F32)]
        + [((5 * count_r, 4 * count_y), F32)] * 2 + [((8, 4 * count_y), F32)] * 2 + [((8, count_y), F32)],
        [pltpu.SemaphoreType.DMA((17,))],
        in_specs=[HBM, HBM],
    )
    got = exchange(p1, p2, p3, p4)
    diagonal = [
        (i * nr + j, ((i + 1) % nx) * nr + (j + 1) % nr) for i in range(nx) for j in range(nr)
    ]
    corner = lax.ppermute(corner, ("group", "rad"), diagonal)
    matrix = ((4 * LANES, 4 * LANES), BF16)
    tiles = pltpu.VMEM((4 * g.halves, 16 * count_r, LANES), F32)
    slim = ((16 * count_r, count_y), F32)
    xd, sd, matrix, *lines = call(
        arrange_kernel(g),
        (x0, source_term),
        [full, full, matrix, full, full, plane, full, slim],
        [tiles],
    )
    outs = [plane, plane, plane, plane, ((16 * count_r, count_y), F32), full, full]
    outs += [plane, plane, edge, edge]
    cx, cxp, cr, crp, cy, inv, z0, *send = call(
        first_kernel(g),
        (xd, sd, *lines, m0, matrix, *got, corner),
        outs,
        [pltpu.VMEM((8 * count_r, 4 * count_y), F32), pltpu.VMEM((16, 4 * count_y), F32), pltpu.VMEM((count_y // 32, 8 * count_r, LANES), F32)],
    )

    def inner(many, with_diagonal, earlier=()):
        rows = count_r if earlier else count_r * len(many)
        return call(
            inner_kernel(g, len(many), with_diagonal, len(earlier)),
            (cx, cxp, cr, crp, cy, inv, matrix, *many, *earlier),
            [full, ((rows, LANES), F32), full] + [full] * with_diagonal,
            [pltpu.VMEM(*full)] * with_diagonal + [tiles],
        )

    def step(vloc, got, earlier, pulls):
        z, *send = call(
            next_kernel(g, pulls),
            (vloc, cx, cr, inv, *got, *earlier),
            [full, plane, plane, edge, edge],
        )
        return z, send

    got = exchange(*send)
    vloc, d0, z0_n, diag_n = inner((z0,), True)
    z1, send = step(vloc, got, (z0,), (SHIFT,))
    got = exchange(*send)
    vloc, d1, z1_n = inner((z0, z1), False)
    z2, send = step(vloc, got, (z1,), (SHIFT,))
    got = exchange(*send)
    vloc, dots, z2_n = inner((z1, z2), False, (d0, d1))
    v3, message = call(
        last_kernel(g, nx * nr),
        (vloc, cx, cr, z2, *got, dots),
        [full, ((nx * nr, LANES), F32)],
    )
    sums = lax.all_to_all(message, ("group", "rad"), 0, 0, tiled=True)
    v3_n, x0 = call(
        restore_kernel(g),
        (v3, guess),
        [full, natural],
        [tiles, pltpu.SemaphoreType.DMA((4,))],
        in_specs=[VMEM, HBM],
        aliases={0: 0},
    )
    return tuple(
        call(
            finish_kernel(g),
            (sums, x0, diag_n, z0_n, z1_n, z2_n, v3_n),
            [natural, natural],
            [pltpu.VMEM(*natural)] * 2 + [pltpu.SemaphoreType.DMA((8,))],
            out_specs=[HBM, HBM],
        )
    )


def solution(mesh):
    in_specs = (P("group", "rad", None), P("group", "rad", None), P(None, "group", "rad", None))
    out_specs = (P("group", "rad", None), P("group", "rad", None))
    return jax.shard_map(steps, mesh=mesh, in_specs=in_specs, out_specs=out_specs, check_vma=False)
```

```python
import math

import jax
import jax.numpy as jnp
import numpy as np
from jax import lax
from jax.experimental import pallas as pl
from jax.experimental.pallas import tpu as pltpu
from jax.sharding import PartitionSpec as P

F32 = jnp.float32
BF16 = jnp.bfloat16
LANES = 128
ROWS = 8
SHIFT = 1.145
DOTS = 5
FOLD = LANES // 2


def gll_tables():
    root = math.sqrt(3.0 / 7.0)
    points = np.array([-1.0, -root, 0.0, root, 1.0])
    weights = np.array([0.1, 49.0 / 90.0, 32.0 / 45.0, 49.0 / 90.0, 0.1])
    factor = np.array(
        [np.prod([points[a] - points[m] for m in range(5) if m != a]) for a in range(5)]
    )
    derivative = np.zeros((5, 5))
    for p in range(5):
        for a in range(5):
            if p == a:
                derivative[p, a] = np.sum(
                    [1.0 / (points[a] - points[m]) for m in range(5) if m != a]
                )
            else:
                derivative[p, a] = factor[p] / (factor[a] * (points[p] - points[a]))
    return derivative, weights


DERIVATIVE, WEIGHTS = gll_tables()
STIFF = DERIVATIVE.T @ np.diag(WEIGHTS) @ DERIVATIVE
K = [[float(v) for v in row] for row in STIFF]
W = [float(v) for v in WEIGHTS]


def line_operator(u):
    u0, u1, u2, u3, u4 = u
    s = u0 if u4 is None else u0 + u4
    o0 = u0 if u4 is None else u0 - u4
    t = u1 + u3
    o1 = u1 - u3
    q = u2 + u2
    d0 = s - q
    d1 = t - q
    e0 = (0.5 * (K[0][0] + K[0][4])) * d0 + (0.5 * (K[0][1] + K[0][3])) * d1
    e1 = (0.5 * (K[1][0] + K[1][4])) * d0 + (0.5 * (K[1][1] + K[1][3])) * d1
    p0 = (0.5 * (K[0][0] - K[0][4])) * o0 + (0.5 * (K[0][1] - K[0][3])) * o1
    p1 = (0.5 * (K[1][0] - K[1][4])) * o0 + (0.5 * (K[1][1] - K[1][3])) * o1
    e = e0 + e1
    return e0 + p0, e1 + p1, -(e + e), e1 - p1, e0 - p0


def last_row(u):
    return K[4][0] * u[0] + K[4][1] * u[1] + K[4][2] * u[2] + K[4][3] * u[3]


class Shape:
    def __init__(self, count_r, count_y):
        self.rows = count_r
        self.halves = count_y // LANES
        self.wide = 4 * LANES

    def row(self, index):
        return pl.ds(self.rows * index, self.rows)

    def lane(self, h, c):
        return pl.ds(self.wide * h + LANES * c, LANES)

    def half(self, h):
        return pl.ds(LANES * h, LANES)


def row_index(g):
    return lax.broadcasted_iota(jnp.int32, (g.rows, LANES), 0)


def lane_index(g):
    return lax.broadcasted_iota(jnp.int32, (g.rows, LANES), 1)


def next_lane(parts, lanes):
    rolled = [pltpu.roll(p, LANES - 1, 1) for p in parts]
    n = len(parts)
    return [jnp.where(lanes == LANES - 1, rolled[(h + 1) % n], rolled[h]) for h in range(n)]


def prev_lane(parts, lanes):
    rolled = [pltpu.roll(p, 1, 1) for p in parts]
    n = len(parts)
    return [jnp.where(lanes == 0, rolled[(h - 1) % n], rolled[h]) for h in range(n)]


def next_row(g, value, rows, last):
    return jnp.where(rows == g.rows - 1, last, pltpu.roll(value, g.rows - 1, 0))


def prev_row(value, rows, first):
    return jnp.where(rows == 0, first, pltpu.roll(value, 1, 0))


def permutation():
    source = lax.broadcasted_iota(jnp.int32, (4 * LANES, 4 * LANES), 0)
    target = lax.broadcasted_iota(jnp.int32, (4 * LANES, 4 * LANES), 1)
    wanted = (target % LANES) * 4 + target // LANES
    return jnp.where(source == wanted, 1.0, 0.0).astype(BF16)


def exact_dot(blocks, matrix, dims):
    parts = []
    for values in blocks:
        one = values.astype(BF16)
        rest = values - one.astype(F32)
        two = rest.astype(BF16)
        three = (rest - two.astype(F32)).astype(BF16)
        parts += [one, two, three]
    product = lax.dot_general(
        jnp.concatenate(parts, 0), matrix, (dims, ((), ())), preferred_element_type=F32
    )
    out = []
    first = 0
    for values in blocks:
        n = values.shape[0]
        one, two, three = (product[first + n * i : first + n * (i + 1)] for i in range(3))
        out.append((one + two) + three)
        first += 3 * n
    return out


def local_apply(g, u_ref, cx, cxp, cr, crp, cy, v_ref):
    rows = row_index(g)
    lanes = lane_index(g)
    for ab in range(16):
        u = [[u_ref[g.row(ab), g.lane(h, c)] for c in range(4)] for h in range(g.halves)]
        fifth = next_lane([u[h][0] for h in range(g.halves)], lanes)
        ends = []
        outs = []
        for h in range(g.halves):
            coef = cy[g.row(ab), g.half(h)]
            r = line_operator(u[h] + [fifth[h]])
            outs.append([coef * r[c] for c in range(4)])
            ends.append(coef * r[4])
        ends = prev_lane(ends, lanes)
        for h in range(g.halves):
            outs[h][0] = outs[h][0] + ends[h]
            for c in range(4):
                v_ref[g.row(ab), g.lane(h, c)] = outs[h][c]
    for h in range(g.halves):
        for c in range(4):
            at = g.lane(h, c)
            u = [[u_ref[g.row(4 * a + b), at] for b in range(4)] for a in range(4)]
            v = [[v_ref[g.row(4 * a + b), at] for b in range(4)] for a in range(4)]
            for b in range(4):
                coef = cx[g.row(b), at]
                r = line_operator([u[a][b] for a in range(4)] + [None])
                for a in range(4):
                    v[a][b] = v[a][b] + coef * r[a]
                v[0][b] = v[0][b] + K[4][4] * (cxp[g.row(b), at] * u[0][b])
            for a in range(4):
                coef = cr[g.row(a), at]
                r = line_operator(u[a] + [next_row(g, u[a][0], rows, 0.0)])
                for b in range(4):
                    v[a][b] = v[a][b] + coef * r[b]
                v[a][0] = v[a][0] + prev_row(coef * r[4], rows, 0.0)
                v[a][0] = v[a][0] + K[4][4] * (crp[g.row(a), at] * u[a][0])
            for a in range(4):
                for b in range(4):
                    v_ref[g.row(4 * a + b), at] = v[a][b]


def add_halo(g, v, coef_x, coef_r, above_x, below_x, above_r, below_r, rows):
    for b in range(4):
        reach = coef_x[b] * above_x[b]
        for a in range(4):
            v[a][b] = v[a][b] + K[a][4] * reach
        v[0][b] = v[0][b] + below_x[b]
    for a in range(4):
        reach = jnp.where(rows == g.rows - 1, coef_r[a] * above_r[a], 0.0)
        for b in range(4):
            v[a][b] = v[a][b] + K[b][4] * reach
        v[a][0] = v[a][0] + jnp.where(rows == 0, below_r[a], 0.0)


def send_planes(g, z, at, h, c, coef_x, coef_r, even_x, even_r, out):
    p1, p2, p3, p4 = out
    for b in range(4):
        down = z[0][b]
        up = coef_x[b] * last_row([z[a][b] for a in range(4)])
        p1[g.row(b), at] = jnp.where(even_x, up, down)
        p2[g.row(b), at] = jnp.where(even_x, down, up)
    for a in range(4):
        down = z[a][0][0:1]
        up = (coef_r[a] * last_row(z[a]))[g.rows - 1 :]
        p3[pl.ds(4 * a + c, 1), g.half(h)] = jnp.where(even_r, up, down)
        p4[pl.ds(4 * a + c, 1), g.half(h)] = jnp.where(even_r, down, up)


def positions():
    ix = lax.axis_index("group")
    ir = lax.axis_index("rad")
    top = ir == lax.axis_size("rad") - 1
    return ix % 2 == 0, ir % 2 == 0, ir == 0, top


def start_kernel(g):
    def body(x_hbm, m_hbm, x_ref, m_ref, p1, p2, p3, p4, corner, sems):
        cut = [(a, g.row(b)) for b in range(4) for a in range(4)]
        copies = [pltpu.make_async_copy(x_hbm.at[at], x_ref.at[at], sems.at[i]) for i, at in enumerate(cut)]
        copies.append(pltpu.make_async_copy(m_hbm, m_ref, sems.at[16]))
        for copy in copies:
            copy.start()
        even_x, even_r, _, _ = positions()
        last = g.rows - 1
        n = 4 * g.rows
        span = LANES * g.halves
        corner[...] = jnp.zeros_like(corner)
        p3[...] = jnp.zeros_like(p3)
        p4[...] = jnp.zeros_like(p4)
        for b in range(4):
            at = g.row(b)
            for copy in copies[4 * b : 4 * b + 4]:
                copy.wait()
            down = x_ref[0, at]
            up = last_row([x_ref[a, at] for a in range(4)])
            p1[at] = jnp.where(even_x, up, down)
            p2[at] = jnp.where(even_x, down, up)
        copies[-1].wait()
        for k in range(3):
            m = m_ref[k, 0]
            p1[pl.ds(n, g.rows), pl.ds(span * k, span)] = m
            p2[pl.ds(n, g.rows), pl.ds(span * k, span)] = m
            edge = m[last:]
            corner[pl.ds(k, 1), :] = edge
            p3[pl.ds(4, 1), pl.ds(span * k, span)] = edge
            p4[pl.ds(4, 1), pl.ds(span * k, span)] = edge
        p1[pl.ds(n, g.rows), pl.ds(span * 3, span)] = m
        p2[pl.ds(n, g.rows), pl.ds(span * 3, span)] = m
        for a in range(4):
            down = x_ref[a, 0:1]
            up = last_row([x_ref[a, pl.ds(4 * last + b, 1)] for b in range(4)])
            p3[pl.ds(a, 1)] = jnp.where(even_r, up, down)
            p4[pl.ds(a, 1)] = jnp.where(even_r, down, up)

    return body


def line_results(g, u_ref, along_x, along_r, end_r, along_y, end_y):
    rows = row_index(g)
    lanes = lane_index(g)
    for ab in range(16):
        u = [[u_ref[g.row(ab), g.lane(h, c)] for c in range(4)] for h in range(g.halves)]
        fifth = next_lane([u[h][0] for h in range(g.halves)], lanes)
        for h in range(g.halves):
            r = line_operator(u[h] + [fifth[h]])
            for c in range(4):
                along_y[g.row(ab), g.lane(h, c)] = r[c]
            end_y[g.row(ab), g.half(h)] = r[4]
    for h in range(g.halves):
        for c in range(4):
            at = g.lane(h, c)
            u = [[u_ref[g.row(4 * a + b), at] for b in range(4)] for a in range(4)]
            for b in range(4):
                r = line_operator([u[a][b] for a in range(4)] + [None])
                for a in range(4):
                    along_x[g.row(4 * a + b), at] = r[a]
            for a in range(4):
                r = line_operator(u[a] + [next_row(g, u[a][0], rows, 0.0)])
                for b in range(4):
                    along_r[g.row(4 * a + b), at] = r[b]
                end_r[g.row(a), at] = r[4]


def arrange_kernel(g):
    def body(x_ref, s_ref, xd, sd, matrix_ref, along_x, along_r, end_r, along_y, end_y, buffer):
        matrix = permutation()
        matrix_ref[...] = matrix
        for source, target in ((x_ref, xd), (s_ref, sd)):
            blocks = [
                source[:, :, pl.ds(g.wide * h, g.wide)].reshape(16 * g.rows, g.wide) for h in range(g.halves)
            ]
            blocks = exact_dot(blocks, matrix, ((1,), (0,)))
            for h in range(g.halves):
                for c in range(4):
                    buffer[4 * h + c] = blocks[h][:, LANES * c : LANES * (c + 1)]
            for h in range(g.halves):
                for c in range(4):
                    for a in range(4):
                        for b in range(4):
                            pick = pl.ds(4 * g.rows * a + b, g.rows, 4)
                            target[g.row(4 * a + b), g.lane(h, c)] = buffer[4 * h + c, pick, :]
        line_results(g, xd, along_x, along_r, end_r, along_y, end_y)

    return body


def first_kernel(g):
    def body(
        xd, sd, along_x, along_r, end_r, along_y, end_y, m_ref, matrix_ref, r1, r2, r3, r4, rc,
        cx, cxp, cr, crp, cy, inv, z_ref, p1, p2, p3, p4,
        planes, edges, buffer,
    ):
        even_x, even_r, bottom, top = positions()
        rows = row_index(g)
        lanes = lane_index(g)
        n = 4 * g.rows
        span = LANES * g.halves
        H = range(g.halves)
        matrix = matrix_ref[...]
        low_all = jnp.where(even_r, r4[4:5, :], r3[4:5, :])
        blocks = []
        for h in H:
            at = pl.ds(g.wide * h, g.wide)
            one, two = r1[0:n, at], r2[0:n, at]
            blocks += [jnp.where(even_x, one, two), jnp.where(even_x, two, one)]
            one, two = r3[:, at], r4[:, at]
            blocks += [jnp.where(even_r, one, two), jnp.where(even_r, two, one)]
        blocks = exact_dot(blocks, matrix, ((1,), (0,)))
        for h in H:
            for c in range(4):
                lanes_c = slice(LANES * c, LANES * (c + 1))
                buffer[4 * h + c, 0:n] = blocks[4 * h][:, lanes_c]
                buffer[4 * h + c, n : 2 * n] = blocks[4 * h + 1][:, lanes_c]
                edges[0:8, g.lane(h, c)] = blocks[4 * h + 2][:, lanes_c]
                edges[8:16, g.lane(h, c)] = blocks[4 * h + 3][:, lanes_c]
            for c in range(4):
                for b in range(4):
                    planes[g.row(b), g.lane(h, c)] = buffer[4 * h + c, pl.ds(b, g.rows, 4), :]
                    planes[g.row(4 + b), g.lane(h, c)] = buffer[4 * h + c, pl.ds(n + b, g.rows, 4), :]
        low = [[jnp.where(bottom, 0.0, low_all[:, span * k + LANES * h : span * k + LANES * (h + 1)]) for h in H] for k in range(3)]
        own = [[m_ref[k, 0, :, g.half(h)] for h in H] for k in range(3)]
        left = []
        for k in range(3):
            pair = []
            for h in H:
                at = pl.ds(span * k + LANES * h, LANES)
                pair.append(jnp.where(even_x, r2[pl.ds(n, g.rows), at], r1[pl.ds(n, g.rows), at]))
            left.append(pair)
        diag_low = [[jnp.where(bottom, 0.0, rc[pl.ds(k, 1), g.half(h)]) for h in H] for k in range(3)]

        def over_y(parts):
            before = prev_lane(parts, lanes)
            return [parts[h] + before[h] for h in H]

        def over_r(parts, edge):
            return [parts[h] + prev_row(parts[h], rows, edge[h]) for h in H]

        def lines_x(parts, edge):
            wide_r = over_r(parts, edge)
            return {(1, 1): parts, (1, 0): over_y(parts), (0, 1): wide_r, (0, 0): over_y(wide_r)}

        for target, table in ((cx, lines_x(own[0], low[0])), (cxp, lines_x(left[0], diag_low[0]))):
            for b in range(4):
                for c in range(4):
                    for h in H:
                        target[g.row(b), g.lane(h, c)] = (W[b] * W[c]) * table[(min(b, 1), min(c, 1))][h]
        zero = [jnp.zeros((g.rows, LANES), F32) for h in H]
        own_r = own[1]
        both_r = [own[1][h] + left[1][h] for h in H]
        table_r = {(1, 1): own_r, (1, 0): over_y(own_r), (0, 1): both_r, (0, 0): over_y(both_r)}
        own_l = [jnp.where(rows == 0, low[1][h], 0.0) for h in H]
        both_l = [jnp.where(rows == 0, low[1][h] + diag_low[1][h], 0.0) for h in H]
        table_l = {(1, 1): own_l, (1, 0): over_y(own_l), (0, 1): both_l, (0, 0): over_y(both_l)}
        for target, table in ((cr, table_r), (crp, table_l)):
            for a in range(4):
                for c in range(4):
                    for h in H:
                        target[g.row(a), g.lane(h, c)] = (W[a] * W[c]) * table[(min(a, 1), min(c, 1))][h]
        both_y = [own[2][h] + left[2][h] for h in H]
        low_y = [low[2][h] + diag_low[2][h] for h in H]
        table_y = {
            (1, 1): own[2],
            (1, 0): over_r(own[2], low[2]),
            (0, 1): both_y,
            (0, 0): over_r(both_y, low_y),
        }
        for a in range(4):
            for b in range(4):
                for h in H:
                    cy[g.row(4 * a + b), g.half(h)] = (W[a] * W[b]) * table_y[(min(a, 1), min(b, 1))][h]
        behind = {}
        for key in table_y:
            behind[key] = prev_lane(table_y[key], lanes)
        for h in H:
            for c in range(4):
                at = g.lane(h, c)
                coef_x = [cx[g.row(b), at] for b in range(4)]
                coef_r = [cr[g.row(a), at] for a in range(4)]
                u = [[xd[g.row(4 * a + b), at] for b in range(4)] for a in range(4)]
                v = [[None] * 4 for _ in range(4)]
                for a in range(4):
                    for b in range(4):
                        rw = g.row(4 * a + b)
                        v[a][b] = coef_x[b] * along_x[rw, at] + coef_r[a] * along_r[rw, at]
                        v[a][b] = v[a][b] + cy[rw, g.half(h)] * along_y[rw, at]
                        if c == 0:
                            ends = [cy[rw, g.half(k)] * end_y[rw, g.half(k)] for k in H]
                            v[a][b] = v[a][b] + prev_lane(ends, lanes)[h]
                    v[a][0] = v[a][0] + prev_row(coef_r[a] * end_r[g.row(a), at], rows, 0.0)
                    v[a][0] = v[a][0] + K[4][4] * (crp[g.row(a), at] * u[a][0])
                for b in range(4):
                    v[0][b] = v[0][b] + K[4][4] * (cxp[g.row(b), at] * u[0][b])
                above_x = [planes[g.row(b), at] for b in range(4)]
                below_x = [cxp[g.row(b), at] * planes[g.row(4 + b), at] for b in range(4)]
                above_r = [jnp.where(top, 0.0, edges[pl.ds(a, 1), at]) for a in range(4)]
                below_r = [jnp.where(bottom, 0.0, crp[pl.ds(g.rows * a, 1), at] * edges[pl.ds(8 + a, 1), at]) for a in range(4)]
                add_halo(g, v, coef_x, coef_r, above_x, below_x, above_r, below_r, rows)
                z = [[None] * 4 for _ in range(4)]
                for a in range(4):
                    for b in range(4):
                        weight = W[a] * W[b]
                        key = (min(a, 1), min(b, 1))
                        diag = K[a][a] * coef_x[b] + K[b][b] * coef_r[a]
                        diag = diag + (K[c][c] * weight) * table_y[key][h]
                        if a == 0:
                            diag = diag + K[4][4] * cxp[g.row(b), at]
                        if b == 0:
                            diag = diag + K[4][4] * prev_row(coef_r[a], rows, crp[pl.ds(g.rows * a, 1), at])
                        if c == 0:
                            diag = diag + (K[4][4] * weight) * behind[key][h]
                        scale = 1.0 / diag
                        r = sd[g.row(4 * a + b), at] - v[a][b]
                        z[a][b] = scale * r
                        inv[g.row(4 * a + b), at] = scale
                        z_ref[g.row(4 * a + b), at] = z[a][b]
                send_planes(g, z, at, h, c, coef_x, coef_r, even_x, even_r, (p1, p2, p3, p4))

    return body


def restore(g, sources, targets, matrix, buffer):
    for source, target in zip(sources, targets):
        for h in range(g.halves):
            for c in range(4):
                for a in range(4):
                    for b in range(4):
                        pick = pl.ds(4 * g.rows * a + b, g.rows, 4)
                        buffer[4 * h + c, pick, :] = source[g.row(4 * a + b), g.lane(h, c)]
        blocks = [jnp.concatenate([buffer[4 * h + c] for c in range(4)], 1) for h in range(g.halves)]
        blocks = exact_dot(blocks, matrix, ((1,), (1,)))
        for h in range(g.halves):
            target[:, pl.ds(g.wide * h, g.wide)] = blocks[h]


def inner_kernel(g, count, with_diagonal, earlier):
    def body(*refs):
        cx, cxp, cr, crp, cy, inv, matrix = refs[:7]
        many = refs[7 : 7 + count]
        before = refs[7 + count : 7 + count + earlier]
        refs = refs[:7] + many + refs[7 + count + earlier :]
        v_ref, dots, z_plain = refs[7 + count : 10 + count]
        buffer = refs[-1]
        newest = many[-1]
        local_apply(g, newest, cx, cxp, cr, crp, cy, v_ref)
        totals = [jnp.zeros((g.rows, LANES), F32)] * count
        diagonal = refs[-2] if with_diagonal else None
        for ab in range(16):
            for h in range(g.halves):
                for c in range(4):
                    at = (g.row(ab), g.lane(h, c))
                    diag = 1.0 / inv[at]
                    if with_diagonal:
                        diagonal[at] = diag
                    weighted = diag * newest[at]
                    totals = [total + weighted * ref[at] for total, ref in zip(totals, many)]
        if earlier:
            parts = [ref[pl.ds(i, g.rows), :] for ref in before for i in range(0, ref.shape[0], g.rows)]
            place = lane_index(g)
            row = jnp.zeros((g.rows, LANES), F32)
            for i, part in enumerate(parts + totals):
                row = row + jnp.where(place == FOLD + i, jnp.sum(part, axis=1, keepdims=True), 0.0)
            dots[...] = jnp.broadcast_to(jnp.sum(row, axis=0, keepdims=True), (g.rows, LANES))
        else:
            for i in range(count):
                dots[pl.ds(g.rows * i, g.rows), :] = totals[i]
        restore(g, [newest], [z_plain], matrix[...], buffer)
        if with_diagonal:
            restore(g, [diagonal], [refs[10 + count]], matrix[...], buffer)

    return body


def received(g, r1, r2, r3, r4, h, c, at, even_x, even_r, bottom, top):
    above_x, below_x, above_r, below_r = [], [], [], []
    for b in range(4):
        one, two = r1[g.row(b), at], r2[g.row(b), at]
        above_x.append(jnp.where(even_x, one, two))
        below_x.append(jnp.where(even_x, two, one))
    for a in range(4):
        one, two = r3[pl.ds(4 * a + c, 1), g.half(h)], r4[pl.ds(4 * a + c, 1), g.half(h)]
        above_r.append(jnp.where(top, 0.0, jnp.where(even_r, one, two)))
        below_r.append(jnp.where(bottom, 0.0, jnp.where(even_r, two, one)))
    return above_x, below_x, above_r, below_r


def next_kernel(g, pulls):
    def body(*refs):
        vloc, cx, cr, inv, r1, r2, r3, r4 = refs[:8]
        earlier = refs[8 : 8 + len(pulls)]
        z_ref, p1, p2, p3, p4 = refs[8 + len(pulls) :]
        even_x, even_r, bottom, top = positions()
        rows = row_index(g)
        for h in range(g.halves):
            for c in range(4):
                at = g.lane(h, c)
                coef_x = [cx[g.row(b), at] for b in range(4)]
                coef_r = [cr[g.row(a), at] for a in range(4)]
                v = [[vloc[g.row(4 * a + b), at] for b in range(4)] for a in range(4)]
                halo = received(g, r1, r2, r3, r4, h, c, at, even_x, even_r, bottom, top)
                add_halo(g, v, coef_x, coef_r, *halo, rows)
                z = [[None] * 4 for _ in range(4)]
                for a in range(4):
                    for b in range(4):
                        rw = g.row(4 * a + b)
                        value = inv[rw, at] * v[a][b]
                        for ref, pull in zip(earlier, pulls):
                            value = value - pull * ref[rw, at]
                        z[a][b] = value
                        z_ref[rw, at] = value
                send_planes(g, z, at, h, c, coef_x, coef_r, even_x, even_r, (p1, p2, p3, p4))

    return body


def last_kernel(g, devices):
    def body(vloc, cx, cr, z_ref, r1, r2, r3, r4, dots, v_ref, message):
        even_x, even_r, bottom, top = positions()
        rows = row_index(g)
        totals = []
        for h in range(g.halves):
            for c in range(4):
                at = g.lane(h, c)
                coef_x = [cx[g.row(b), at] for b in range(4)]
                coef_r = [cr[g.row(a), at] for a in range(4)]
                v = [[vloc[g.row(4 * a + b), at] for b in range(4)] for a in range(4)]
                halo = received(g, r1, r2, r3, r4, h, c, at, even_x, even_r, bottom, top)
                add_halo(g, v, coef_x, coef_r, *halo, rows)
                for a in range(4):
                    total = jnp.zeros((g.rows, LANES), F32)
                    for b in range(4):
                        rw = g.row(4 * a + b)
                        v_ref[rw, at] = v[a][b]
                        total = total + z_ref[rw, at] * v[a][b]
                    totals.append(total)
        while len(totals) > 1:
            totals = [sum(totals[i : i + 2]) for i in range(0, len(totals), 2)]
        row = jnp.sum(totals[0], axis=0, keepdims=True)
        row = row + pltpu.roll(row, FOLD, 1)
        place = lax.broadcasted_iota(jnp.int32, (1, LANES), 1)
        row = jnp.where(place < FOLD, row, dots[0:1])
        message[...] = jnp.broadcast_to(row, (devices, LANES))

    return body


def finish_kernel(g):
    def body(sums, x_ref, diag, z0, z1, z2, v_ref, matrix, solution_hbm, residual_hbm, solution_ref, residual_ref, v3, buffer, sems):
        total = jnp.sum(sums[...], axis=0, keepdims=True)
        place = lax.broadcasted_iota(jnp.int32, (1, LANES), 1)
        picks = [place == FOLD + i for i in range(DOTS)] + [place < FOLD]
        dot = [jnp.sum(jnp.where(pick, total, 0.0), axis=1, keepdims=True) for pick in picks]
        s00, s01, s11, s12, s22, m22 = dot
        m00 = s01 + SHIFT * s00
        m01 = s11 + SHIFT * s01
        m02 = s12 + SHIFT * s11
        m11 = m02
        m12 = s22 + SHIFT * s12
        l10 = m01 / m00
        l20 = m02 / m00
        d1 = m11 - l10 * m01
        t = m12 - l10 * m02
        l21 = t / d1
        d2 = m22 - l20 * m02 - l21 * t
        y1 = s01 - l10 * s00
        y2 = s11 - l20 * s00 - l21 * y1
        c2 = y2 / d2
        c1 = y1 / d1 - l21 * c2
        c0 = s00 / m00 - l10 * c1 - l20 * c2
        e0 = 1.0 - SHIFT * c0
        e1 = c0 + SHIFT * c1
        copies = []
        cuts = [(a, pl.ds(4 * g.rows * b, 4 * g.rows)) for a in range(4) for b in range(4 // 4)]
        rows = [pl.ds(4 * g.rows * i, 4 * g.rows) for i in range(len(cuts))]
        for n, (to, at) in enumerate(zip(cuts, rows)):
            solution_ref[to] = x_ref[to] + (c0 * z0[at] + (c1 * z1[at] + c2 * z2[at]))
            copies.append(pltpu.make_async_copy(solution_ref.at[to], solution_hbm.at[to], sems.at[n]))
            copies[-1].start()
        restore(g, [v_ref], [v3], matrix[...], buffer)
        for n, (to, at) in enumerate(zip(cuts, rows)):
            residual_ref[to] = diag[at] * (e0 * z0[at] - (e1 * z1[at] + c1 * z2[at])) - c2 * v3[at]
            copies.append(pltpu.make_async_copy(residual_ref.at[to], residual_hbm.at[to], sems.at[len(cuts) + n]))
            copies[-1].start()
        for copy in copies:
            copy.wait()

    return body


def swaps(count, parity):
    pairs = []
    for i in range(count):
        step = 1 if i % 2 == parity else -1
        pairs.append((i, (i + step) % count))
    return pairs


VMEM = pl.BlockSpec(memory_space=pltpu.VMEM)
HBM = pl.BlockSpec(memory_space=pltpu.HBM)
MIB = 1024 * 1024


def call(body, args, outs, scratch=(), limit=6, in_specs=None, out_specs=None, aliases=None, flops=1000000):
    return pl.pallas_call(
        body,
        in_specs=in_specs or [VMEM] * len(args),
        out_specs=out_specs or [VMEM] * len(outs),
        out_shape=[jax.ShapeDtypeStruct(s, t) for s, t in outs],
        scratch_shapes=list(scratch),
        input_output_aliases=aliases or {},
        cost_estimate=pl.CostEstimate(flops=flops, bytes_accessed=1000000, transcendentals=0),
        compiler_params=pltpu.CompilerParams(vmem_limit_bytes=limit * MIB),
    )(*args)


def steps(source_term, initial_guess, metric):
    count_x, count_r, count_y = metric.shape[1:]
    assert count_x == 1 and count_r == ROWS and count_y % LANES == 0
    g = Shape(count_r, count_y)
    nx, nr = lax.axis_size("group"), lax.axis_size("rad")
    assert nx % 2 == 0 and nr % 2 == 0
    full = ((16 * count_r, 4 * count_y), F32)
    plane = ((4 * count_r, 4 * count_y), F32)
    edge = ((16, count_y), F32)
    natural = (initial_guess.shape, F32)

    def exchange(p1, p2, p3, p4):
        sends = ((p1, "group", nx, 0), (p2, "group", nx, 1), (p3, "rad", nr, 0), (p4, "rad", nr, 1))
        got = []
        for value, axis, count, parity in sends:
            got.append(lax.ppermute(value, axis, swaps(count, parity)))
        return tuple(got)

    guess = pltpu.with_memory_space_constraint(initial_guess, pltpu.HBM)
    x0, m0, p1, p2, p3, p4, corner = call(
        start_kernel(g),
        (guess, pltpu.with_memory_space_constraint(metric, pltpu.HBM)),
        [natural, (metric.shape, F32)]
        + [((5 * count_r, 4 * count_y), F32)] * 2 + [((8, 4 * count_y), F32)] * 2 + [((8, count_y), F32)],
        [pltpu.SemaphoreType.DMA((17,))],
        in_specs=[HBM, HBM],
    )
    got = exchange(p1, p2, p3, p4)
    diagonal = [
        (i * nr + j, ((i + 1) % nx) * nr + (j + 1) % nr) for i in range(nx) for j in range(nr)
    ]
    corner = lax.ppermute(corner, ("group", "rad"), diagonal)
    matrix = ((4 * LANES, 4 * LANES), BF16)
    tiles = pltpu.VMEM((4 * g.halves, 16 * count_r, LANES), F32)
    slim = ((16 * count_r, count_y), F32)
    xd, sd, matrix, *lines = call(
        arrange_kernel(g),
        (x0, source_term),
        [full, full, matrix, full, full, plane, full, slim],
        [tiles],
    )
    outs = [plane, plane, plane, plane, ((16 * count_r, count_y), F32), full, full]
    outs += [plane, plane, edge, edge]
    cx, cxp, cr, crp, cy, inv, z0, *send = call(
        first_kernel(g),
        (xd, sd, *lines, m0, matrix, *got, corner),
        outs,
        [pltpu.VMEM((8 * count_r, 4 * count_y), F32), pltpu.VMEM((16, 4 * count_y), F32), pltpu.VMEM((count_y // 32, 8 * count_r, LANES), F32)],
    )

    def inner(many, with_diagonal, earlier=()):
        rows = count_r if earlier else count_r * len(many)
        return call(
            inner_kernel(g, len(many), with_diagonal, len(earlier)),
            (cx, cxp, cr, crp, cy, inv, matrix, *many, *earlier),
            [full, ((rows, LANES), F32), full] + [full] * with_diagonal,
            [pltpu.VMEM(*full)] * with_diagonal + [tiles],
        )

    def step(vloc, got, earlier, pulls):
        z, *send = call(
            next_kernel(g, pulls),
            (vloc, cx, cr, inv, *got, *earlier),
            [full, plane, plane, edge, edge],
        )
        return z, send

    got = exchange(*send)
    vloc, d0, z0_n, diag_n = inner((z0,), True)
    z1, send = step(vloc, got, (z0,), (SHIFT,))
    got = exchange(*send)
    vloc, d1, z1_n = inner((z0, z1), False)
    z2, send = step(vloc, got, (z1,), (SHIFT,))
    got = exchange(*send)
    vloc, dots, z2_n = inner((z1, z2), False, (d0, d1))
    v3, message = call(
        last_kernel(g, nx * nr),
        (vloc, cx, cr, z2, *got, dots),
        [full, ((nx * nr, LANES), F32)],
    )
    sums = lax.all_to_all(message, ("group", "rad"), 0, 0, tiled=True)
    return tuple(
        call(
            finish_kernel(g),
            (sums, x0, diag_n, z0_n, z1_n, z2_n, v3, matrix),
            [natural, natural],
            [pltpu.VMEM(*natural)] * 2 + [pltpu.VMEM(*full), tiles, pltpu.SemaphoreType.DMA((8,))],
            out_specs=[HBM, HBM],
        )
    )


def solution(mesh):
    in_specs = (P("group", "rad", None), P("group", "rad", None), P(None, "group", "rad", None))
    out_specs = (P("group", "rad", None), P("group", "rad", None))
    return jax.shard_map(steps, mesh=mesh, in_specs=in_specs, out_specs=out_specs, check_vma=False)
```

```python
import math

import jax
import jax.numpy as jnp
import numpy as np
from jax import lax
from jax.experimental import pallas as pl
from jax.experimental.pallas import tpu as pltpu
from jax.sharding import PartitionSpec as P

F32 = jnp.float32
BF16 = jnp.bfloat16
LANES = 128
ROWS = 8
DOTS = 5
FOLD = LANES // 2


def gll_tables():
    root = math.sqrt(3.0 / 7.0)
    points = np.array([-1.0, -root, 0.0, root, 1.0])
    weights = np.array([0.1, 49.0 / 90.0, 32.0 / 45.0, 49.0 / 90.0, 0.1])
    factor = np.array(
        [np.prod([points[a] - points[m] for m in range(5) if m != a]) for a in range(5)]
    )
    derivative = np.zeros((5, 5))
    for p in range(5):
        for a in range(5):
            if p == a:
                derivative[p, a] = np.sum(
                    [1.0 / (points[a] - points[m]) for m in range(5) if m != a]
                )
            else:
                derivative[p, a] = factor[p] / (factor[a] * (points[p] - points[a]))
    return derivative, weights


DERIVATIVE, WEIGHTS = gll_tables()
STIFF = DERIVATIVE.T @ np.diag(WEIGHTS) @ DERIVATIVE
K = [[float(v) for v in row] for row in STIFF]
W = [float(v) for v in WEIGHTS]


def line_operator(u):
    u0, u1, u2, u3, u4 = u
    s = u0 if u4 is None else u0 + u4
    o0 = u0 if u4 is None else u0 - u4
    t = u1 + u3
    o1 = u1 - u3
    q = u2 + u2
    d0 = s - q
    d1 = t - q
    e0 = (0.5 * (K[0][0] + K[0][4])) * d0 + (0.5 * (K[0][1] + K[0][3])) * d1
    e1 = (0.5 * (K[1][0] + K[1][4])) * d0 + (0.5 * (K[1][1] + K[1][3])) * d1
    p0 = (0.5 * (K[0][0] - K[0][4])) * o0 + (0.5 * (K[0][1] - K[0][3])) * o1
    p1 = (0.5 * (K[1][0] - K[1][4])) * o0 + (0.5 * (K[1][1] - K[1][3])) * o1
    e = e0 + e1
    return e0 + p0, e1 + p1, -(e + e), e1 - p1, e0 - p0


def last_row(u):
    return K[4][0] * u[0] + K[4][1] * u[1] + K[4][2] * u[2] + K[4][3] * u[3]


def tree_sum(values):
    while len(values) > 1:
        pairs = [values[i] + values[i + 1] for i in range(0, len(values) - 1, 2)]
        values = pairs + values[len(values) - len(values) % 2 :]
    return values[0]


class Shape:
    def __init__(self, count_r, count_y):
        self.rows = count_r
        self.halves = count_y // LANES
        self.wide = 4 * LANES

    def row(self, index):
        return pl.ds(self.rows * index, self.rows)

    def lane(self, h, c):
        return pl.ds(self.wide * h + LANES * c, LANES)

    def half(self, h):
        return pl.ds(LANES * h, LANES)


def row_index(g):
    return lax.broadcasted_iota(jnp.int32, (g.rows, LANES), 0)


def lane_index(g):
    return lax.broadcasted_iota(jnp.int32, (g.rows, LANES), 1)


def next_lane(parts, lanes):
    rolled = [pltpu.roll(p, LANES - 1, 1) for p in parts]
    n = len(parts)
    return [jnp.where(lanes == LANES - 1, rolled[(h + 1) % n], rolled[h]) for h in range(n)]


def prev_lane(parts, lanes):
    rolled = [pltpu.roll(p, 1, 1) for p in parts]
    n = len(parts)
    return [jnp.where(lanes == 0, rolled[(h - 1) % n], rolled[h]) for h in range(n)]


def next_row(g, value, rows, last):
    return jnp.where(rows == g.rows - 1, last, pltpu.roll(value, g.rows - 1, 0))


def prev_row(value, rows, first):
    return jnp.where(rows == 0, first, pltpu.roll(value, 1, 0))


def permutation():
    source = lax.broadcasted_iota(jnp.int32, (4 * LANES, 4 * LANES), 0)
    target = lax.broadcasted_iota(jnp.int32, (4 * LANES, 4 * LANES), 1)
    wanted = (target % LANES) * 4 + target // LANES
    return jnp.where(source == wanted, 1.0, 0.0).astype(BF16)


def exact_dot(blocks, matrix, dims):
    parts = []
    for values in blocks:
        one = values.astype(BF16)
        rest = values - one.astype(F32)
        two = rest.astype(BF16)
        three = (rest - two.astype(F32)).astype(BF16)
        parts += [one, two, three]
    product = lax.dot_general(
        jnp.concatenate(parts, 0), matrix, (dims, ((), ())), preferred_element_type=F32
    )
    out = []
    first = 0
    for values in blocks:
        n = values.shape[0]
        one, two, three = (product[first + n * i : first + n * (i + 1)] for i in range(3))
        out.append((one + two) + three)
        first += 3 * n
    return out


def local_apply(g, u_ref, cx, cxp, cr, crp, cy, v_ref):
    rows = row_index(g)
    lanes = lane_index(g)
    for ab in range(16):
        u = [[u_ref[g.row(ab), g.lane(h, c)] for c in range(4)] for h in range(g.halves)]
        fifth = next_lane([u[h][0] for h in range(g.halves)], lanes)
        ends = []
        outs = []
        for h in range(g.halves):
            coef = cy[g.row(ab), g.half(h)]
            r = line_operator(u[h] + [fifth[h]])
            outs.append([coef * r[c] for c in range(4)])
            ends.append(coef * r[4])
        ends = prev_lane(ends, lanes)
        for h in range(g.halves):
            outs[h][0] = outs[h][0] + ends[h]
            for c in range(4):
                v_ref[g.row(ab), g.lane(h, c)] = outs[h][c]
    for h in range(g.halves):
        for c in range(4):
            at = g.lane(h, c)
            u = [[u_ref[g.row(4 * a + b), at] for b in range(4)] for a in range(4)]
            v = [[v_ref[g.row(4 * a + b), at] for b in range(4)] for a in range(4)]
            for b in range(4):
                coef = cx[g.row(b), at]
                r = line_operator([u[a][b] for a in range(4)] + [None])
                for a in range(4):
                    v[a][b] = v[a][b] + coef * r[a]
                v[0][b] = v[0][b] + K[4][4] * (cxp[g.row(b), at] * u[0][b])
            for a in range(4):
                coef = cr[g.row(a), at]
                r = line_operator(u[a] + [next_row(g, u[a][0], rows, 0.0)])
                for b in range(4):
                    v[a][b] = v[a][b] + coef * r[b]
                v[a][0] = v[a][0] + prev_row(coef * r[4], rows, 0.0)
                v[a][0] = v[a][0] + K[4][4] * (crp[g.row(a), at] * u[a][0])
            for a in range(4):
                for b in range(4):
                    v_ref[g.row(4 * a + b), at] = v[a][b]


def add_halo(g, v, coef_x, coef_r, above_x, below_x, above_r, below_r, rows):
    for b in range(4):
        reach = coef_x[b] * above_x[b]
        for a in range(4):
            v[a][b] = v[a][b] + K[a][4] * reach
        v[0][b] = v[0][b] + below_x[b]
    for a in range(4):
        reach = jnp.where(rows == g.rows - 1, coef_r[a] * above_r[a], 0.0)
        for b in range(4):
            v[a][b] = v[a][b] + K[b][4] * reach
        v[a][0] = v[a][0] + jnp.where(rows == 0, below_r[a], 0.0)


def send_planes(g, z, at, h, c, coef_x, coef_r, even_x, even_r, out):
    p1, p2, p3, p4 = out
    for b in range(4):
        down = z[0][b]
        up = coef_x[b] * last_row([z[a][b] for a in range(4)])
        p1[g.row(b), at] = jnp.where(even_x, up, down)
        p2[g.row(b), at] = jnp.where(even_x, down, up)
    for a in range(4):
        down = z[a][0][0:1]
        up = (coef_r[a] * last_row(z[a]))[g.rows - 1 :]
        p3[pl.ds(4 * a + c, 1), g.half(h)] = jnp.where(even_r, up, down)
        p4[pl.ds(4 * a + c, 1), g.half(h)] = jnp.where(even_r, down, up)


def positions():
    ix = lax.axis_index("group")
    ir = lax.axis_index("rad")
    top = ir == lax.axis_size("rad") - 1
    return ix % 2 == 0, ir % 2 == 0, ir == 0, top


def start_kernel(g):
    def body(x_hbm, m_hbm, x_ref, m_ref, p1, p2, p3, p4, corner, sems):
        cut = [(a, g.row(b)) for b in range(4) for a in range(4)]
        copies = [pltpu.make_async_copy(x_hbm.at[at], x_ref.at[at], sems.at[i]) for i, at in enumerate(cut)]
        copies.append(pltpu.make_async_copy(m_hbm, m_ref, sems.at[16]))
        for copy in copies:
            copy.start()
        even_x, even_r, _, _ = positions()
        last = g.rows - 1
        n = 4 * g.rows
        span = LANES * g.halves
        corner[...] = jnp.zeros_like(corner)
        p3[...] = jnp.zeros_like(p3)
        p4[...] = jnp.zeros_like(p4)
        for b in range(4):
            at = g.row(b)
            for copy in copies[4 * b : 4 * b + 4]:
                copy.wait()
            down = x_ref[0, at]
            up = last_row([x_ref[a, at] for a in range(4)])
            p1[at] = jnp.where(even_x, up, down)
            p2[at] = jnp.where(even_x, down, up)
        copies[-1].wait()
        for k in range(3):
            m = m_ref[k, 0]
            p1[pl.ds(n, g.rows), pl.ds(span * k, span)] = m
            p2[pl.ds(n, g.rows), pl.ds(span * k, span)] = m
            edge = m[last:]
            corner[pl.ds(k, 1), :] = edge
            p3[pl.ds(4, 1), pl.ds(span * k, span)] = edge
            p4[pl.ds(4, 1), pl.ds(span * k, span)] = edge
        p1[pl.ds(n, g.rows), pl.ds(span * 3, span)] = m
        p2[pl.ds(n, g.rows), pl.ds(span * 3, span)] = m
        for a in range(4):
            down = x_ref[a, 0:1]
            up = last_row([x_ref[a, pl.ds(4 * last + b, 1)] for b in range(4)])
            p3[pl.ds(a, 1)] = jnp.where(even_r, up, down)
            p4[pl.ds(a, 1)] = jnp.where(even_r, down, up)

    return body


def line_results(g, u_ref, along_x, along_r, end_r, along_y, end_y):
    rows = row_index(g)
    lanes = lane_index(g)
    for ab in range(16):
        u = [[u_ref[g.row(ab), g.lane(h, c)] for c in range(4)] for h in range(g.halves)]
        fifth = next_lane([u[h][0] for h in range(g.halves)], lanes)
        for h in range(g.halves):
            r = line_operator(u[h] + [fifth[h]])
            for c in range(4):
                along_y[g.row(ab), g.lane(h, c)] = r[c]
            end_y[g.row(ab), g.half(h)] = r[4]
    for h in range(g.halves):
        for c in range(4):
            at = g.lane(h, c)
            u = [[u_ref[g.row(4 * a + b), at] for b in range(4)] for a in range(4)]
            for b in range(4):
                r = line_operator([u[a][b] for a in range(4)] + [None])
                for a in range(4):
                    along_x[g.row(4 * a + b), at] = r[a]
            for a in range(4):
                r = line_operator(u[a] + [next_row(g, u[a][0], rows, 0.0)])
                for b in range(4):
                    along_r[g.row(4 * a + b), at] = r[b]
                end_r[g.row(a), at] = r[4]


def arrange_kernel(g):
    def body(x_ref, s_ref, xd, sd, matrix_ref, along_x, along_r, end_r, along_y, end_y, buffer):
        matrix = permutation()
        matrix_ref[...] = matrix
        for source, target in ((x_ref, xd), (s_ref, sd)):
            blocks = [
                source[:, :, pl.ds(g.wide * h, g.wide)].reshape(16 * g.rows, g.wide) for h in range(g.halves)
            ]
            blocks = exact_dot(blocks, matrix, ((1,), (0,)))
            for h in range(g.halves):
                for c in range(4):
                    buffer[4 * h + c] = blocks[h][:, LANES * c : LANES * (c + 1)]
            for h in range(g.halves):
                for c in range(4):
                    for a in range(4):
                        for b in range(4):
                            pick = pl.ds(4 * g.rows * a + b, g.rows, 4)
                            target[g.row(4 * a + b), g.lane(h, c)] = buffer[4 * h + c, pick, :]
        line_results(g, xd, along_x, along_r, end_r, along_y, end_y)

    return body


def first_kernel(g):
    def body(
        xd, sd, along_x, along_r, end_r, along_y, end_y, m_ref, matrix_ref, r1, r2, r3, r4, rc,
        cx, cxp, cr, crp, cy, inv, z_ref, p1, p2, p3, p4,
        planes, edges, buffer,
    ):
        even_x, even_r, bottom, top = positions()
        rows = row_index(g)
        lanes = lane_index(g)
        n = 4 * g.rows
        span = LANES * g.halves
        H = range(g.halves)
        matrix = matrix_ref[...]
        low_all = jnp.where(even_r, r4[4:5, :], r3[4:5, :])
        blocks = []
        for h in H:
            at = pl.ds(g.wide * h, g.wide)
            one, two = r1[0:n, at], r2[0:n, at]
            blocks += [jnp.where(even_x, one, two), jnp.where(even_x, two, one)]
            one, two = r3[:, at], r4[:, at]
            blocks += [jnp.where(even_r, one, two), jnp.where(even_r, two, one)]
        blocks = exact_dot(blocks, matrix, ((1,), (0,)))
        for h in H:
            for c in range(4):
                lanes_c = slice(LANES * c, LANES * (c + 1))
                buffer[4 * h + c, 0:n] = blocks[4 * h][:, lanes_c]
                buffer[4 * h + c, n : 2 * n] = blocks[4 * h + 1][:, lanes_c]
                edges[0:8, g.lane(h, c)] = blocks[4 * h + 2][:, lanes_c]
                edges[8:16, g.lane(h, c)] = blocks[4 * h + 3][:, lanes_c]
            for c in range(4):
                for b in range(4):
                    planes[g.row(b), g.lane(h, c)] = buffer[4 * h + c, pl.ds(b, g.rows, 4), :]
                    planes[g.row(4 + b), g.lane(h, c)] = buffer[4 * h + c, pl.ds(n + b, g.rows, 4), :]
        low = [[jnp.where(bottom, 0.0, low_all[:, span * k + LANES * h : span * k + LANES * (h + 1)]) for h in H] for k in range(3)]
        own = [[m_ref[k, 0, :, g.half(h)] for h in H] for k in range(3)]
        left = []
        for k in range(3):
            pair = []
            for h in H:
                at = pl.ds(span * k + LANES * h, LANES)
                pair.append(jnp.where(even_x, r2[pl.ds(n, g.rows), at], r1[pl.ds(n, g.rows), at]))
            left.append(pair)
        diag_low = [[jnp.where(bottom, 0.0, rc[pl.ds(k, 1), g.half(h)]) for h in H] for k in range(3)]

        def over_y(parts):
            before = prev_lane(parts, lanes)
            return [parts[h] + before[h] for h in H]

        def over_r(parts, edge):
            return [parts[h] + prev_row(parts[h], rows, edge[h]) for h in H]

        def lines_x(parts, edge):
            wide_r = over_r(parts, edge)
            return {(1, 1): parts, (1, 0): over_y(parts), (0, 1): wide_r, (0, 0): over_y(wide_r)}

        for target, table in ((cx, lines_x(own[0], low[0])), (cxp, lines_x(left[0], diag_low[0]))):
            for b in range(4):
                for c in range(4):
                    for h in H:
                        target[g.row(b), g.lane(h, c)] = (W[b] * W[c]) * table[(min(b, 1), min(c, 1))][h]
        zero = [jnp.zeros((g.rows, LANES), F32) for h in H]
        own_r = own[1]
        both_r = [own[1][h] + left[1][h] for h in H]
        table_r = {(1, 1): own_r, (1, 0): over_y(own_r), (0, 1): both_r, (0, 0): over_y(both_r)}
        own_l = [jnp.where(rows == 0, low[1][h], 0.0) for h in H]
        both_l = [jnp.where(rows == 0, low[1][h] + diag_low[1][h], 0.0) for h in H]
        table_l = {(1, 1): own_l, (1, 0): over_y(own_l), (0, 1): both_l, (0, 0): over_y(both_l)}
        for target, table in ((cr, table_r), (crp, table_l)):
            for a in range(4):
                for c in range(4):
                    for h in H:
                        target[g.row(a), g.lane(h, c)] = (W[a] * W[c]) * table[(min(a, 1), min(c, 1))][h]
        both_y = [own[2][h] + left[2][h] for h in H]
        low_y = [low[2][h] + diag_low[2][h] for h in H]
        table_y = {
            (1, 1): own[2],
            (1, 0): over_r(own[2], low[2]),
            (0, 1): both_y,
            (0, 0): over_r(both_y, low_y),
        }
        for a in range(4):
            for b in range(4):
                for h in H:
                    cy[g.row(4 * a + b), g.half(h)] = (W[a] * W[b]) * table_y[(min(a, 1), min(b, 1))][h]
        behind = {}
        for key in table_y:
            behind[key] = prev_lane(table_y[key], lanes)
        for h in H:
            for c in range(4):
                at = g.lane(h, c)
                coef_x = [cx[g.row(b), at] for b in range(4)]
                coef_r = [cr[g.row(a), at] for a in range(4)]
                u = [[xd[g.row(4 * a + b), at] for b in range(4)] for a in range(4)]
                v = [[None] * 4 for _ in range(4)]
                for a in range(4):
                    for b in range(4):
                        rw = g.row(4 * a + b)
                        v[a][b] = coef_x[b] * along_x[rw, at] + coef_r[a] * along_r[rw, at]
                        v[a][b] = v[a][b] + cy[rw, g.half(h)] * along_y[rw, at]
                        if c == 0:
                            ends = [cy[rw, g.half(k)] * end_y[rw, g.half(k)] for k in H]
                            v[a][b] = v[a][b] + prev_lane(ends, lanes)[h]
                    v[a][0] = v[a][0] + prev_row(coef_r[a] * end_r[g.row(a), at], rows, 0.0)
                    v[a][0] = v[a][0] + K[4][4] * (crp[g.row(a), at] * u[a][0])
                for b in range(4):
                    v[0][b] = v[0][b] + K[4][4] * (cxp[g.row(b), at] * u[0][b])
                above_x = [planes[g.row(b), at] for b in range(4)]
                below_x = [cxp[g.row(b), at] * planes[g.row(4 + b), at] for b in range(4)]
                above_r = [jnp.where(top, 0.0, edges[pl.ds(a, 1), at]) for a in range(4)]
                below_r = [jnp.where(bottom, 0.0, crp[pl.ds(g.rows * a, 1), at] * edges[pl.ds(8 + a, 1), at]) for a in range(4)]
                add_halo(g, v, coef_x, coef_r, above_x, below_x, above_r, below_r, rows)
                z = [[None] * 4 for _ in range(4)]
                for a in range(4):
                    for b in range(4):
                        weight = W[a] * W[b]
                        key = (min(a, 1), min(b, 1))
                        diag = K[a][a] * coef_x[b] + K[b][b] * coef_r[a]
                        diag = diag + (K[c][c] * weight) * table_y[key][h]
                        if a == 0:
                            diag = diag + K[4][4] * cxp[g.row(b), at]
                        if b == 0:
                            diag = diag + K[4][4] * prev_row(coef_r[a], rows, crp[pl.ds(g.rows * a, 1), at])
                        if c == 0:
                            diag = diag + (K[4][4] * weight) * behind[key][h]
                        scale = 1.0 / diag
                        r = sd[g.row(4 * a + b), at] - v[a][b]
                        z[a][b] = scale * r
                        inv[g.row(4 * a + b), at] = scale
                        z_ref[g.row(4 * a + b), at] = z[a][b]
                send_planes(g, z, at, h, c, coef_x, coef_r, even_x, even_r, (p1, p2, p3, p4))

    return body


def restore(g, sources, targets, matrix, buffer):
    for source, target in zip(sources, targets):
        for h in range(g.halves):
            for c in range(4):
                for a in range(4):
                    for b in range(4):
                        pick = pl.ds(4 * g.rows * a + b, g.rows, 4)
                        buffer[4 * h + c, pick, :] = source[g.row(4 * a + b), g.lane(h, c)]
        blocks = [jnp.concatenate([buffer[4 * h + c] for c in range(4)], 1) for h in range(g.halves)]
        blocks = exact_dot(blocks, matrix, ((1,), (1,)))
        for h in range(g.halves):
            target[:, pl.ds(g.wide * h, g.wide)] = blocks[h]


def inner_kernel(g, count, with_diagonal, earlier):
    def body(*refs):
        cx, cxp, cr, crp, cy, inv, matrix = refs[:7]
        many = refs[7 : 7 + count]
        before = refs[7 + count : 7 + count + earlier]
        refs = refs[:7] + many + refs[7 + count + earlier :]
        v_ref, dots, z_plain = refs[7 + count : 10 + count]
        buffer = refs[-1]
        newest = many[-1]
        local_apply(g, newest, cx, cxp, cr, crp, cy, v_ref)
        terms = [[] for _ in range(count)]
        diagonal = refs[-2] if with_diagonal else None
        for ab in range(16):
            group = [[] for _ in range(count)]
            for h in range(g.halves):
                for c in range(4):
                    at = (g.row(ab), g.lane(h, c))
                    diag = 1.0 / inv[at]
                    if with_diagonal:
                        diagonal[at] = diag
                    weighted = diag * newest[at]
                    for values, ref in zip(group, many):
                        values.append(weighted * ref[at])
            for values, part in zip(terms, group):
                values.append(tree_sum(part))
        totals = [tree_sum(values) for values in terms]
        if earlier:
            parts = [ref[pl.ds(i, g.rows), :] for ref in before for i in range(0, ref.shape[0], g.rows)]
            place = lane_index(g)
            row = jnp.zeros((g.rows, LANES), F32)
            for i, part in enumerate(parts + totals):
                row = row + jnp.where(place == FOLD + i, jnp.sum(part, axis=1, keepdims=True), 0.0)
            dots[...] = jnp.broadcast_to(jnp.sum(row, axis=0, keepdims=True), (g.rows, LANES))
        else:
            for i in range(count):
                dots[pl.ds(g.rows * i, g.rows), :] = totals[i]
        restore(g, [newest], [z_plain], matrix[...], buffer)
        if with_diagonal:
            restore(g, [diagonal], [refs[10 + count]], matrix[...], buffer)

    return body


def received(g, r1, r2, r3, r4, h, c, at, even_x, even_r, bottom, top):
    above_x, below_x, above_r, below_r = [], [], [], []
    for b in range(4):
        one, two = r1[g.row(b), at], r2[g.row(b), at]
        above_x.append(jnp.where(even_x, one, two))
        below_x.append(jnp.where(even_x, two, one))
    for a in range(4):
        one, two = r3[pl.ds(4 * a + c, 1), g.half(h)], r4[pl.ds(4 * a + c, 1), g.half(h)]
        above_r.append(jnp.where(top, 0.0, jnp.where(even_r, one, two)))
        below_r.append(jnp.where(bottom, 0.0, jnp.where(even_r, two, one)))
    return above_x, below_x, above_r, below_r


def next_kernel(g):
    def body(*refs):
        vloc, cx, cr, inv, r1, r2, r3, r4 = refs[:8]
        z_ref, p1, p2, p3, p4 = refs[8:]
        even_x, even_r, bottom, top = positions()
        rows = row_index(g)
        for h in range(g.halves):
            for c in range(4):
                at = g.lane(h, c)
                coef_x = [cx[g.row(b), at] for b in range(4)]
                coef_r = [cr[g.row(a), at] for a in range(4)]
                v = [[vloc[g.row(4 * a + b), at] for b in range(4)] for a in range(4)]
                halo = received(g, r1, r2, r3, r4, h, c, at, even_x, even_r, bottom, top)
                add_halo(g, v, coef_x, coef_r, *halo, rows)
                z = [[None] * 4 for _ in range(4)]
                for a in range(4):
                    for b in range(4):
                        rw = g.row(4 * a + b)
                        z[a][b] = inv[rw, at] * v[a][b]
                        z_ref[rw, at] = z[a][b]
                send_planes(g, z, at, h, c, coef_x, coef_r, even_x, even_r, (p1, p2, p3, p4))

    return body


def last_kernel(g, devices):
    def body(vloc, cx, cr, z_ref, r1, r2, r3, r4, dots, v_ref, message):
        even_x, even_r, bottom, top = positions()
        rows = row_index(g)
        totals = []
        for h in range(g.halves):
            for c in range(4):
                at = g.lane(h, c)
                coef_x = [cx[g.row(b), at] for b in range(4)]
                coef_r = [cr[g.row(a), at] for a in range(4)]
                v = [[vloc[g.row(4 * a + b), at] for b in range(4)] for a in range(4)]
                halo = received(g, r1, r2, r3, r4, h, c, at, even_x, even_r, bottom, top)
                add_halo(g, v, coef_x, coef_r, *halo, rows)
                for a in range(4):
                    for b in range(4):
                        v_ref[g.row(4 * a + b), at] = v[a][b]
                    totals.append(tree_sum([z_ref[g.row(4 * a + b), at] * v[a][b] for b in range(4)]))
        row = jnp.sum(tree_sum(totals), axis=0, keepdims=True)
        row = row + pltpu.roll(row, FOLD, 1)
        place = lax.broadcasted_iota(jnp.int32, (1, LANES), 1)
        row = jnp.where(place < FOLD, row, dots[0:1])
        message[...] = jnp.broadcast_to(row, (devices, LANES))

    return body


def finish_kernel(g):
    def body(sums, x_ref, diag, z0, z1, z2, v_ref, matrix, solution_hbm, residual_hbm, solution_ref, residual_ref, v3, buffer, sems):
        total = jnp.sum(sums[...], axis=0, keepdims=True)
        place = lax.broadcasted_iota(jnp.int32, (1, LANES), 1)
        picks = [place == FOLD + i for i in range(DOTS)] + [place < FOLD]
        dot = [jnp.sum(jnp.where(pick, total, 0.0), axis=1, keepdims=True) for pick in picks]
        s00, s01, s11, s12, s22, m22 = dot
        m00, m01, m02, m11, m12 = s01, s11, s12, s12, s22
        l10 = m01 / m00
        l20 = m02 / m00
        d1 = m11 - l10 * m01
        t = m12 - l10 * m02
        l21 = t / d1
        d2 = m22 - l20 * m02 - l21 * t
        y1 = s01 - l10 * s00
        y2 = s11 - l20 * s00 - l21 * y1
        c2 = y2 / d2
        c1 = y1 / d1 - l21 * c2
        c0 = s00 / m00 - l10 * c1 - l20 * c2
        copies = []
        cuts = [(a, pl.ds(4 * g.rows * b, 4 * g.rows)) for a in range(4) for b in range(4 // 4)]
        rows = [pl.ds(4 * g.rows * i, 4 * g.rows) for i in range(len(cuts))]
        for n, (to, at) in enumerate(zip(cuts, rows)):
            solution_ref[to] = x_ref[to] + (c0 * z0[at] + (c1 * z1[at] + c2 * z2[at]))
            copies.append(pltpu.make_async_copy(solution_ref.at[to], solution_hbm.at[to], sems.at[n]))
            copies[-1].start()
        restore(g, [v_ref], [v3], matrix[...], buffer)
        for n, (to, at) in enumerate(zip(cuts, rows)):
            residual_ref[to] = diag[at] * (z0[at] - (c0 * z1[at] + c1 * z2[at])) - c2 * v3[at]
            copies.append(pltpu.make_async_copy(residual_ref.at[to], residual_hbm.at[to], sems.at[len(cuts) + n]))
            copies[-1].start()
        for copy in copies:
            copy.wait()

    return body


def swaps(count, parity):
    pairs = []
    for i in range(count):
        step = 1 if i % 2 == parity else -1
        pairs.append((i, (i + step) % count))
    return pairs


VMEM = pl.BlockSpec(memory_space=pltpu.VMEM)
HBM = pl.BlockSpec(memory_space=pltpu.HBM)
MIB = 1024 * 1024


def call(body, args, outs, scratch=(), limit=6, in_specs=None, out_specs=None, aliases=None, flops=1000000):
    return pl.pallas_call(
        body,
        in_specs=in_specs or [VMEM] * len(args),
        out_specs=out_specs or [VMEM] * len(outs),
        out_shape=[jax.ShapeDtypeStruct(s, t) for s, t in outs],
        scratch_shapes=list(scratch),
        input_output_aliases=aliases or {},
        cost_estimate=pl.CostEstimate(flops=flops, bytes_accessed=1000000, transcendentals=0),
        compiler_params=pltpu.CompilerParams(vmem_limit_bytes=limit * MIB),
    )(*args)


def steps(source_term, initial_guess, metric):
    count_x, count_r, count_y = metric.shape[1:]
    assert count_x == 1 and count_r == ROWS and count_y % LANES == 0
    g = Shape(count_r, count_y)
    nx, nr = lax.axis_size("group"), lax.axis_size("rad")
    assert nx % 2 == 0 and nr % 2 == 0
    full = ((16 * count_r, 4 * count_y), F32)
    plane = ((4 * count_r, 4 * count_y), F32)
    edge = ((16, count_y), F32)
    natural = (initial_guess.shape, F32)

    def exchange(p1, p2, p3, p4):
        sends = ((p1, "group", nx, 0), (p2, "group", nx, 1), (p3, "rad", nr, 0), (p4, "rad", nr, 1))
        got = []
        for value, axis, count, parity in sends:
            got.append(lax.ppermute(value, axis, swaps(count, parity)))
        return tuple(got)

    guess = pltpu.with_memory_space_constraint(initial_guess, pltpu.HBM)
    x0, m0, p1, p2, p3, p4, corner = call(
        start_kernel(g),
        (guess, pltpu.with_memory_space_constraint(metric, pltpu.HBM)),
        [natural, (metric.shape, F32)]
        + [((5 * count_r, 4 * count_y), F32)] * 2 + [((8, 4 * count_y), F32)] * 2 + [((8, count_y), F32)],
        [pltpu.SemaphoreType.DMA((17,))],
        in_specs=[HBM, HBM],
    )
    got = exchange(p1, p2, p3, p4)
    diagonal = [
        (i * nr + j, ((i + 1) % nx) * nr + (j + 1) % nr) for i in range(nx) for j in range(nr)
    ]
    corner = lax.ppermute(corner, ("group", "rad"), diagonal)
    matrix = ((4 * LANES, 4 * LANES), BF16)
    tiles = pltpu.VMEM((4 * g.halves, 16 * count_r, LANES), F32)
    slim = ((16 * count_r, count_y), F32)
    xd, sd, matrix, *lines = call(
        arrange_kernel(g),
        (x0, source_term),
        [full, full, matrix, full, full, plane, full, slim],
        [tiles],
    )
    outs = [plane, plane, plane, plane, ((16 * count_r, count_y), F32), full, full]
    outs += [plane, plane, edge, edge]
    cx, cxp, cr, crp, cy, inv, z0, *send = call(
        first_kernel(g),
        (xd, sd, *lines, m0, matrix, *got, corner),
        outs,
        [pltpu.VMEM((8 * count_r, 4 * count_y), F32), pltpu.VMEM((16, 4 * count_y), F32), pltpu.VMEM((count_y // 32, 8 * count_r, LANES), F32)],
    )

    def inner(many, with_diagonal, earlier=()):
        rows = count_r if earlier else count_r * len(many)
        return call(
            inner_kernel(g, len(many), with_diagonal, len(earlier)),
            (cx, cxp, cr, crp, cy, inv, matrix, *many, *earlier),
            [full, ((rows, LANES), F32), full] + [full] * with_diagonal,
            [pltpu.VMEM(*full)] * with_diagonal + [tiles],
        )

    def step(vloc, got):
        z, *send = call(
            next_kernel(g),
            (vloc, cx, cr, inv, *got),
            [full, plane, plane, edge, edge],
        )
        return z, send

    got = exchange(*send)
    vloc, d0, z0_n, diag_n = inner((z0,), True)
    z1, send = step(vloc, got)
    got = exchange(*send)
    vloc, d1, z1_n = inner((z0, z1), False)
    z2, send = step(vloc, got)
    got = exchange(*send)
    vloc, dots, z2_n = inner((z1, z2), False, (d0, d1))
    v3, message = call(
        last_kernel(g, nx * nr),
        (vloc, cx, cr, z2, *got, dots),
        [full, ((nx * nr, LANES), F32)],
    )
    sums = lax.all_to_all(message, ("group", "rad"), 0, 0, tiled=True)
    return tuple(
        call(
            finish_kernel(g),
            (sums, x0, diag_n, z0_n, z1_n, z2_n, v3, matrix),
            [natural, natural],
            [pltpu.VMEM(*natural)] * 2 + [pltpu.VMEM(*full), tiles, pltpu.SemaphoreType.DMA((8,))],
            out_specs=[HBM, HBM],
        )
    )


def solution(mesh):
    in_specs = (P("group", "rad", None), P("group", "rad", None), P(None, "group", "rad", None))
    out_specs = (P("group", "rad", None), P("group", "rad", None))
    return jax.shard_map(steps, mesh=mesh, in_specs=in_specs, out_specs=out_specs, check_vma=False)
```

```python
import math

import jax
import jax.numpy as jnp
import numpy as np
from jax import lax
from jax.experimental import pallas as pl
from jax.experimental.pallas import tpu as pltpu
from jax.sharding import PartitionSpec as P

F32 = jnp.float32
BF16 = jnp.bfloat16
LANES = 128
ROWS = 8
SHIFT = 0.5
DOTS = 5
FOLD = LANES // 2


def gll_tables():
    root = math.sqrt(3.0 / 7.0)
    points = np.array([-1.0, -root, 0.0, root, 1.0])
    weights = np.array([0.1, 49.0 / 90.0, 32.0 / 45.0, 49.0 / 90.0, 0.1])
    factor = np.array(
        [np.prod([points[a] - points[m] for m in range(5) if m != a]) for a in range(5)]
    )
    derivative = np.zeros((5, 5))
    for p in range(5):
        for a in range(5):
            if p == a:
                derivative[p, a] = np.sum(
                    [1.0 / (points[a] - points[m]) for m in range(5) if m != a]
                )
            else:
                derivative[p, a] = factor[p] / (factor[a] * (points[p] - points[a]))
    return derivative, weights


DERIVATIVE, WEIGHTS = gll_tables()
STIFF = DERIVATIVE.T @ np.diag(WEIGHTS) @ DERIVATIVE
K = [[float(v) for v in row] for row in STIFF]
W = [float(v) for v in WEIGHTS]


def line_operator(u):
    u0, u1, u2, u3, u4 = u
    s = u0 if u4 is None else u0 + u4
    o0 = u0 if u4 is None else u0 - u4
    t = u1 + u3
    o1 = u1 - u3
    q = u2 + u2
    d0 = s - q
    d1 = t - q
    e0 = (0.5 * (K[0][0] + K[0][4])) * d0 + (0.5 * (K[0][1] + K[0][3])) * d1
    e1 = (0.5 * (K[1][0] + K[1][4])) * d0 + (0.5 * (K[1][1] + K[1][3])) * d1
    p0 = (0.5 * (K[0][0] - K[0][4])) * o0 + (0.5 * (K[0][1] - K[0][3])) * o1
    p1 = (0.5 * (K[1][0] - K[1][4])) * o0 + (0.5 * (K[1][1] - K[1][3])) * o1
    e = e0 + e1
    return e0 + p0, e1 + p1, -(e + e), e1 - p1, e0 - p0


def last_row(u):
    return K[4][0] * u[0] + K[4][1] * u[1] + K[4][2] * u[2] + K[4][3] * u[3]


def tree_sum(values):
    while len(values) > 1:
        pairs = [values[i] + values[i + 1] for i in range(0, len(values) - 1, 2)]
        values = pairs + values[len(values) - len(values) % 2 :]
    return values[0]


class Shape:
    def __init__(self, count_r, count_y):
        self.rows = count_r
        self.halves = count_y // LANES
        self.wide = 4 * LANES

    def row(self, index):
        return pl.ds(self.rows * index, self.rows)

    def lane(self, h, c):
        return pl.ds(self.wide * h + LANES * c, LANES)

    def half(self, h):
        return pl.ds(LANES * h, LANES)


def row_index(g):
    return lax.broadcasted_iota(jnp.int32, (g.rows, LANES), 0)


def lane_index(g):
    return lax.broadcasted_iota(jnp.int32, (g.rows, LANES), 1)


def next_lane(parts, lanes):
    rolled = [pltpu.roll(p, LANES - 1, 1) for p in parts]
    n = len(parts)
    return [jnp.where(lanes == LANES - 1, rolled[(h + 1) % n], rolled[h]) for h in range(n)]


def prev_lane(parts, lanes):
    rolled = [pltpu.roll(p, 1, 1) for p in parts]
    n = len(parts)
    return [jnp.where(lanes == 0, rolled[(h - 1) % n], rolled[h]) for h in range(n)]


def next_row(g, value, rows, last):
    return jnp.where(rows == g.rows - 1, last, pltpu.roll(value, g.rows - 1, 0))


def prev_row(value, rows, first):
    return jnp.where(rows == 0, first, pltpu.roll(value, 1, 0))


def permutation():
    source = lax.broadcasted_iota(jnp.int32, (4 * LANES, 4 * LANES), 0)
    target = lax.broadcasted_iota(jnp.int32, (4 * LANES, 4 * LANES), 1)
    wanted = (target % LANES) * 4 + target // LANES
    return jnp.where(source == wanted, 1.0, 0.0).astype(BF16)


def exact_dot(blocks, matrix, dims):
    parts = []
    for values in blocks:
        one = values.astype(BF16)
        rest = values - one.astype(F32)
        two = rest.astype(BF16)
        three = (rest - two.astype(F32)).astype(BF16)
        parts += [one, two, three]
    product = lax.dot_general(
        jnp.concatenate(parts, 0), matrix, (dims, ((), ())), preferred_element_type=F32
    )
    out = []
    first = 0
    for values in blocks:
        n = values.shape[0]
        one, two, three = (product[first + n * i : first + n * (i + 1)] for i in range(3))
        out.append((one + two) + three)
        first += 3 * n
    return out


def local_apply(g, u_ref, cx, cxp, cr, crp, cy, v_ref):
    rows = row_index(g)
    lanes = lane_index(g)
    for ab in range(16):
        u = [[u_ref[g.row(ab), g.lane(h, c)] for c in range(4)] for h in range(g.halves)]
        fifth = next_lane([u[h][0] for h in range(g.halves)], lanes)
        ends = []
        outs = []
        for h in range(g.halves):
            coef = cy[g.row(ab), g.half(h)]
            r = line_operator(u[h] + [fifth[h]])
            outs.append([coef * r[c] for c in range(4)])
            ends.append(coef * r[4])
        ends = prev_lane(ends, lanes)
        for h in range(g.halves):
            outs[h][0] = outs[h][0] + ends[h]
            for c in range(4):
                v_ref[g.row(ab), g.lane(h, c)] = outs[h][c]
    for h in range(g.halves):
        for c in range(4):
            at = g.lane(h, c)
            u = [[u_ref[g.row(4 * a + b), at] for b in range(4)] for a in range(4)]
            v = [[v_ref[g.row(4 * a + b), at] for b in range(4)] for a in range(4)]
            for b in range(4):
                coef = cx[g.row(b), at]
                r = line_operator([u[a][b] for a in range(4)] + [None])
                for a in range(4):
                    v[a][b] = v[a][b] + coef * r[a]
                v[0][b] = v[0][b] + K[4][4] * (cxp[g.row(b), at] * u[0][b])
            for a in range(4):
                coef = cr[g.row(a), at]
                r = line_operator(u[a] + [next_row(g, u[a][0], rows, 0.0)])
                for b in range(4):
                    v[a][b] = v[a][b] + coef * r[b]
                v[a][0] = v[a][0] + prev_row(coef * r[4], rows, 0.0)
                v[a][0] = v[a][0] + K[4][4] * (crp[g.row(a), at] * u[a][0])
            for a in range(4):
                for b in range(4):
                    v_ref[g.row(4 * a + b), at] = v[a][b]


def add_halo(g, v, coef_x, coef_r, above_x, below_x, above_r, below_r, rows):
    for b in range(4):
        reach = coef_x[b] * above_x[b]
        for a in range(4):
            v[a][b] = v[a][b] + K[a][4] * reach
        v[0][b] = v[0][b] + below_x[b]
    for a in range(4):
        reach = jnp.where(rows == g.rows - 1, coef_r[a] * above_r[a], 0.0)
        for b in range(4):
            v[a][b] = v[a][b] + K[b][4] * reach
        v[a][0] = v[a][0] + jnp.where(rows == 0, below_r[a], 0.0)


def send_planes(g, z, at, h, c, coef_x, coef_r, even_x, even_r, out):
    p1, p2, p3, p4 = out
    for b in range(4):
        down = z[0][b]
        up = coef_x[b] * last_row([z[a][b] for a in range(4)])
        p1[g.row(b), at] = jnp.where(even_x, up, down)
        p2[g.row(b), at] = jnp.where(even_x, down, up)
    for a in range(4):
        down = z[a][0][0:1]
        up = (coef_r[a] * last_row(z[a]))[g.rows - 1 :]
        p3[pl.ds(4 * a + c, 1), g.half(h)] = jnp.where(even_r, up, down)
        p4[pl.ds(4 * a + c, 1), g.half(h)] = jnp.where(even_r, down, up)


def positions():
    ix = lax.axis_index("group")
    ir = lax.axis_index("rad")
    top = ir == lax.axis_size("rad") - 1
    return ix % 2 == 0, ir % 2 == 0, ir == 0, top


def start_kernel(g):
    def body(x_hbm, m_hbm, x_ref, m_ref, p1, p2, p3, p4, corner, sems):
        cut = [(a, g.row(b)) for b in range(4) for a in range(4)]
        copies = [pltpu.make_async_copy(x_hbm.at[at], x_ref.at[at], sems.at[i]) for i, at in enumerate(cut)]
        copies.append(pltpu.make_async_copy(m_hbm, m_ref, sems.at[16]))
        for copy in copies:
            copy.start()
        even_x, even_r, _, _ = positions()
        last = g.rows - 1
        n = 4 * g.rows
        span = LANES * g.halves
        corner[...] = jnp.zeros_like(corner)
        p3[...] = jnp.zeros_like(p3)
        p4[...] = jnp.zeros_like(p4)
        for b in range(4):
            at = g.row(b)
            for copy in copies[4 * b : 4 * b + 4]:
                copy.wait()
            down = x_ref[0, at]
            up = last_row([x_ref[a, at] for a in range(4)])
            p1[at] = jnp.where(even_x, up, down)
            p2[at] = jnp.where(even_x, down, up)
        copies[-1].wait()
        for k in range(3):
            m = m_ref[k, 0]
            p1[pl.ds(n, g.rows), pl.ds(span * k, span)] = m
            p2[pl.ds(n, g.rows), pl.ds(span * k, span)] = m
            edge = m[last:]
            corner[pl.ds(k, 1), :] = edge
            p3[pl.ds(4, 1), pl.ds(span * k, span)] = edge
            p4[pl.ds(4, 1), pl.ds(span * k, span)] = edge
        p1[pl.ds(n, g.rows), pl.ds(span * 3, span)] = m
        p2[pl.ds(n, g.rows), pl.ds(span * 3, span)] = m
        for a in range(4):
            down = x_ref[a, 0:1]
            up = last_row([x_ref[a, pl.ds(4 * last + b, 1)] for b in range(4)])
            p3[pl.ds(a, 1)] = jnp.where(even_r, up, down)
            p4[pl.ds(a, 1)] = jnp.where(even_r, down, up)

    return body


def line_results(g, u_ref, along_x, along_r, end_r, along_y, end_y):
    rows = row_index(g)
    lanes = lane_index(g)
    for ab in range(16):
        u = [[u_ref[g.row(ab), g.lane(h, c)] for c in range(4)] for h in range(g.halves)]
        fifth = next_lane([u[h][0] for h in range(g.halves)], lanes)
        for h in range(g.halves):
            r = line_operator(u[h] + [fifth[h]])
            for c in range(4):
                along_y[g.row(ab), g.lane(h, c)] = r[c]
            end_y[g.row(ab), g.half(h)] = r[4]
    for h in range(g.halves):
        for c in range(4):
            at = g.lane(h, c)
            u = [[u_ref[g.row(4 * a + b), at] for b in range(4)] for a in range(4)]
            for b in range(4):
                r = line_operator([u[a][b] for a in range(4)] + [None])
                for a in range(4):
                    along_x[g.row(4 * a + b), at] = r[a]
            for a in range(4):
                r = line_operator(u[a] + [next_row(g, u[a][0], rows, 0.0)])
                for b in range(4):
                    along_r[g.row(4 * a + b), at] = r[b]
                end_r[g.row(a), at] = r[4]


def arrange_kernel(g):
    def body(x_ref, s_ref, xd, sd, matrix_ref, along_x, along_r, end_r, along_y, end_y, buffer):
        matrix = permutation()
        matrix_ref[...] = matrix
        for source, target in ((x_ref, xd), (s_ref, sd)):
            blocks = [
                source[:, :, pl.ds(g.wide * h, g.wide)].reshape(16 * g.rows, g.wide) for h in range(g.halves)
            ]
            blocks = exact_dot(blocks, matrix, ((1,), (0,)))
            for h in range(g.halves):
                for c in range(4):
                    buffer[4 * h + c] = blocks[h][:, LANES * c : LANES * (c + 1)]
            for h in range(g.halves):
                for c in range(4):
                    for a in range(4):
                        for b in range(4):
                            pick = pl.ds(4 * g.rows * a + b, g.rows, 4)
                            target[g.row(4 * a + b), g.lane(h, c)] = buffer[4 * h + c, pick, :]
        line_results(g, xd, along_x, along_r, end_r, along_y, end_y)

    return body


def first_kernel(g):
    def body(
        xd, sd, along_x, along_r, end_r, along_y, end_y, m_ref, matrix_ref, r1, r2, r3, r4, rc,
        cx, cxp, cr, crp, cy, inv, z_ref, p1, p2, p3, p4,
        planes, edges, buffer,
    ):
        even_x, even_r, bottom, top = positions()
        rows = row_index(g)
        lanes = lane_index(g)
        n = 4 * g.rows
        span = LANES * g.halves
        H = range(g.halves)
        matrix = matrix_ref[...]
        low_all = jnp.where(even_r, r4[4:5, :], r3[4:5, :])
        blocks = []
        for h in H:
            at = pl.ds(g.wide * h, g.wide)
            one, two = r1[0:n, at], r2[0:n, at]
            blocks += [jnp.where(even_x, one, two), jnp.where(even_x, two, one)]
            one, two = r3[:, at], r4[:, at]
            blocks += [jnp.where(even_r, one, two), jnp.where(even_r, two, one)]
        blocks = exact_dot(blocks, matrix, ((1,), (0,)))
        for h in H:
            for c in range(4):
                lanes_c = slice(LANES * c, LANES * (c + 1))
                buffer[4 * h + c, 0:n] = blocks[4 * h][:, lanes_c]
                buffer[4 * h + c, n : 2 * n] = blocks[4 * h + 1][:, lanes_c]
                edges[0:8, g.lane(h, c)] = blocks[4 * h + 2][:, lanes_c]
                edges[8:16, g.lane(h, c)] = blocks[4 * h + 3][:, lanes_c]
            for c in range(4):
                for b in range(4):
                    planes[g.row(b), g.lane(h, c)] = buffer[4 * h + c, pl.ds(b, g.rows, 4), :]
                    planes[g.row(4 + b), g.lane(h, c)] = buffer[4 * h + c, pl.ds(n + b, g.rows, 4), :]
        low = [[jnp.where(bottom, 0.0, low_all[:, span * k + LANES * h : span * k + LANES * (h + 1)]) for h in H] for k in range(3)]
        own = [[m_ref[k, 0, :, g.half(h)] for h in H] for k in range(3)]
        left = []
        for k in range(3):
            pair = []
            for h in H:
                at = pl.ds(span * k + LANES * h, LANES)
                pair.append(jnp.where(even_x, r2[pl.ds(n, g.rows), at], r1[pl.ds(n, g.rows), at]))
            left.append(pair)
        diag_low = [[jnp.where(bottom, 0.0, rc[pl.ds(k, 1), g.half(h)]) for h in H] for k in range(3)]

        def over_y(parts):
            before = prev_lane(parts, lanes)
            return [parts[h] + before[h] for h in H]

        def over_r(parts, edge):
            return [parts[h] + prev_row(parts[h], rows, edge[h]) for h in H]

        def lines_x(parts, edge):
            wide_r = over_r(parts, edge)
            return {(1, 1): parts, (1, 0): over_y(parts), (0, 1): wide_r, (0, 0): over_y(wide_r)}

        for target, table in ((cx, lines_x(own[0], low[0])), (cxp, lines_x(left[0], diag_low[0]))):
            for b in range(4):
                for c in range(4):
                    for h in H:
                        target[g.row(b), g.lane(h, c)] = (W[b] * W[c]) * table[(min(b, 1), min(c, 1))][h]
        zero = [jnp.zeros((g.rows, LANES), F32) for h in H]
        own_r = own[1]
        both_r = [own[1][h] + left[1][h] for h in H]
        table_r = {(1, 1): own_r, (1, 0): over_y(own_r), (0, 1): both_r, (0, 0): over_y(both_r)}
        own_l = [jnp.where(rows == 0, low[1][h], 0.0) for h in H]
        both_l = [jnp.where(rows == 0, low[1][h] + diag_low[1][h], 0.0) for h in H]
        table_l = {(1, 1): own_l, (1, 0): over_y(own_l), (0, 1): both_l, (0, 0): over_y(both_l)}
        for target, table in ((cr, table_r), (crp, table_l)):
            for a in range(4):
                for c in range(4):
                    for h in H:
                        target[g.row(a), g.lane(h, c)] = (W[a] * W[c]) * table[(min(a, 1), min(c, 1))][h]
        both_y = [own[2][h] + left[2][h] for h in H]
        low_y = [low[2][h] + diag_low[2][h] for h in H]
        table_y = {
            (1, 1): own[2],
            (1, 0): over_r(own[2], low[2]),
            (0, 1): both_y,
            (0, 0): over_r(both_y, low_y),
        }
        for a in range(4):
            for b in range(4):
                for h in H:
                    cy[g.row(4 * a + b), g.half(h)] = (W[a] * W[b]) * table_y[(min(a, 1), min(b, 1))][h]
        behind = {}
        for key in table_y:
            behind[key] = prev_lane(table_y[key], lanes)
        for h in H:
            for c in range(4):
                at = g.lane(h, c)
                coef_x = [cx[g.row(b), at] for b in range(4)]
                coef_r = [cr[g.row(a), at] for a in range(4)]
                u = [[xd[g.row(4 * a + b), at] for b in range(4)] for a in range(4)]
                v = [[None] * 4 for _ in range(4)]
                for a in range(4):
                    for b in range(4):
                        rw = g.row(4 * a + b)
                        v[a][b] = coef_x[b] * along_x[rw, at] + coef_r[a] * along_r[rw, at]
                        v[a][b] = v[a][b] + cy[rw, g.half(h)] * along_y[rw, at]
                        if c == 0:
                            ends = [cy[rw, g.half(k)] * end_y[rw, g.half(k)] for k in H]
                            v[a][b] = v[a][b] + prev_lane(ends, lanes)[h]
                    v[a][0] = v[a][0] + prev_row(coef_r[a] * end_r[g.row(a), at], rows, 0.0)
                    v[a][0] = v[a][0] + K[4][4] * (crp[g.row(a), at] * u[a][0])
                for b in range(4):
                    v[0][b] = v[0][b] + K[4][4] * (cxp[g.row(b), at] * u[0][b])
                above_x = [planes[g.row(b), at] for b in range(4)]
                below_x = [cxp[g.row(b), at] * planes[g.row(4 + b), at] for b in range(4)]
                above_r = [jnp.where(top, 0.0, edges[pl.ds(a, 1), at]) for a in range(4)]
                below_r = [jnp.where(bottom, 0.0, crp[pl.ds(g.rows * a, 1), at] * edges[pl.ds(8 + a, 1), at]) for a in range(4)]
                add_halo(g, v, coef_x, coef_r, above_x, below_x, above_r, below_r, rows)
                z = [[None] * 4 for _ in range(4)]
                for a in range(4):
                    for b in range(4):
                        weight = W[a] * W[b]
                        key = (min(a, 1), min(b, 1))
                        diag = K[a][a] * coef_x[b] + K[b][b] * coef_r[a]
                        diag = diag + (K[c][c] * weight) * table_y[key][h]
                        if a == 0:
                            diag = diag + K[4][4] * cxp[g.row(b), at]
                        if b == 0:
                            diag = diag + K[4][4] * prev_row(coef_r[a], rows, crp[pl.ds(g.rows * a, 1), at])
                        if c == 0:
                            diag = diag + (K[4][4] * weight) * behind[key][h]
                        scale = 1.0 / diag
                        r = sd[g.row(4 * a + b), at] - v[a][b]
                        z[a][b] = scale * r
                        inv[g.row(4 * a + b), at] = scale
                        z_ref[g.row(4 * a + b), at] = z[a][b]
                send_planes(g, z, at, h, c, coef_x, coef_r, even_x, even_r, (p1, p2, p3, p4))

    return body


def restore(g, sources, targets, matrix, buffer):
    for source, target in zip(sources, targets):
        for h in range(g.halves):
            for c in range(4):
                for a in range(4):
                    for b in range(4):
                        pick = pl.ds(4 * g.rows * a + b, g.rows, 4)
                        buffer[4 * h + c, pick, :] = source[g.row(4 * a + b), g.lane(h, c)]
        blocks = [jnp.concatenate([buffer[4 * h + c] for c in range(4)], 1) for h in range(g.halves)]
        blocks = exact_dot(blocks, matrix, ((1,), (1,)))
        for h in range(g.halves):
            target[:, pl.ds(g.wide * h, g.wide)] = blocks[h]


def inner_kernel(g, count, with_diagonal, earlier):
    def body(*refs):
        cx, cxp, cr, crp, cy, inv, matrix = refs[:7]
        many = refs[7 : 7 + count]
        before = refs[7 + count : 7 + count + earlier]
        refs = refs[:7] + many + refs[7 + count + earlier :]
        v_ref, dots, z_plain = refs[7 + count : 10 + count]
        buffer = refs[-1]
        newest = many[-1]
        local_apply(g, newest, cx, cxp, cr, crp, cy, v_ref)
        terms = [[] for _ in range(count)]
        diagonal = refs[-2] if with_diagonal else None
        for ab in range(16):
            group = [[] for _ in range(count)]
            for h in range(g.halves):
                for c in range(4):
                    at = (g.row(ab), g.lane(h, c))
                    diag = 1.0 / inv[at]
                    if with_diagonal:
                        diagonal[at] = diag
                    weighted = diag * newest[at]
                    for values, ref in zip(group, many):
                        values.append(weighted * ref[at])
            for values, part in zip(terms, group):
                values.append(tree_sum(part))
        totals = [tree_sum(values) for values in terms]
        if earlier:
            parts = [ref[pl.ds(i, g.rows), :] for ref in before for i in range(0, ref.shape[0], g.rows)]
            place = lane_index(g)
            row = jnp.zeros((g.rows, LANES), F32)
            for i, part in enumerate(parts + totals):
                row = row + jnp.where(place == FOLD + i, jnp.sum(part, axis=1, keepdims=True), 0.0)
            dots[...] = jnp.broadcast_to(jnp.sum(row, axis=0, keepdims=True), (g.rows, LANES))
        else:
            for i in range(count):
                dots[pl.ds(g.rows * i, g.rows), :] = totals[i]
        restore(g, [newest], [z_plain], matrix[...], buffer)
        if with_diagonal:
            restore(g, [diagonal], [refs[10 + count]], matrix[...], buffer)

    return body


def received(g, r1, r2, r3, r4, h, c, at, even_x, even_r, bottom, top):
    above_x, below_x, above_r, below_r = [], [], [], []
    for b in range(4):
        one, two = r1[g.row(b), at], r2[g.row(b), at]
        above_x.append(jnp.where(even_x, one, two))
        below_x.append(jnp.where(even_x, two, one))
    for a in range(4):
        one, two = r3[pl.ds(4 * a + c, 1), g.half(h)], r4[pl.ds(4 * a + c, 1), g.half(h)]
        above_r.append(jnp.where(top, 0.0, jnp.where(even_r, one, two)))
        below_r.append(jnp.where(bottom, 0.0, jnp.where(even_r, two, one)))
    return above_x, below_x, above_r, below_r


def next_kernel(g, pulls):
    def body(*refs):
        vloc, cx, cr, inv, r1, r2, r3, r4 = refs[:8]
        earlier = refs[8 : 8 + len(pulls)]
        z_ref, p1, p2, p3, p4 = refs[8 + len(pulls) :]
        even_x, even_r, bottom, top = positions()
        rows = row_index(g)
        for h in range(g.halves):
            for c in range(4):
                at = g.lane(h, c)
                coef_x = [cx[g.row(b), at] for b in range(4)]
                coef_r = [cr[g.row(a), at] for a in range(4)]
                v = [[vloc[g.row(4 * a + b), at] for b in range(4)] for a in range(4)]
                halo = received(g, r1, r2, r3, r4, h, c, at, even_x, even_r, bottom, top)
                add_halo(g, v, coef_x, coef_r, *halo, rows)
                z = [[None] * 4 for _ in range(4)]
                for a in range(4):
                    for b in range(4):
                        rw = g.row(4 * a + b)
                        value = inv[rw, at] * v[a][b]
                        for ref, pull in zip(earlier, pulls):
                            value = value - pull * ref[rw, at]
                        z[a][b] = value
                        z_ref[rw, at] = value
                send_planes(g, z, at, h, c, coef_x, coef_r, even_x, even_r, (p1, p2, p3, p4))

    return body


def last_kernel(g, devices):
    def body(vloc, cx, cr, z_ref, r1, r2, r3, r4, dots, v_ref, message):
        even_x, even_r, bottom, top = positions()
        rows = row_index(g)
        totals = []
        for h in range(g.halves):
            for c in range(4):
                at = g.lane(h, c)
                coef_x = [cx[g.row(b), at] for b in range(4)]
                coef_r = [cr[g.row(a), at] for a in range(4)]
                v = [[vloc[g.row(4 * a + b), at] for b in range(4)] for a in range(4)]
                halo = received(g, r1, r2, r3, r4, h, c, at, even_x, even_r, bottom, top)
                add_halo(g, v, coef_x, coef_r, *halo, rows)
                for a in range(4):
                    for b in range(4):
                        v_ref[g.row(4 * a + b), at] = v[a][b]
                    totals.append(tree_sum([z_ref[g.row(4 * a + b), at] * v[a][b] for b in range(4)]))
        row = jnp.sum(tree_sum(totals), axis=0, keepdims=True)
        row = row + pltpu.roll(row, FOLD, 1)
        place = lax.broadcasted_iota(jnp.int32, (1, LANES), 1)
        row = jnp.where(place < FOLD, row, dots[0:1])
        message[...] = jnp.broadcast_to(row, (devices, LANES))

    return body


def finish_kernel(g):
    def body(sums, x_ref, diag, z0, z1, z2, v_ref, matrix, solution_hbm, residual_hbm, solution_ref, residual_ref, v3, buffer, sems):
        total = jnp.sum(sums[...], axis=0, keepdims=True)
        place = lax.broadcasted_iota(jnp.int32, (1, LANES), 1)
        picks = [place == FOLD + i for i in range(DOTS)] + [place < FOLD]
        dot = [jnp.sum(jnp.where(pick, total, 0.0), axis=1, keepdims=True) for pick in picks]
        s00, s01, s11, s12, s22, m22 = dot
        m00 = s01 + SHIFT * s00
        m01 = s11 + SHIFT * s01
        m02 = s12 + SHIFT * s11
        m11 = m02
        m12 = s22 + SHIFT * s12
        l10 = m01 / m00
        l20 = m02 / m00
        d1 = m11 - l10 * m01
        t = m12 - l10 * m02
        l21 = t / d1
        d2 = m22 - l20 * m02 - l21 * t
        y1 = s01 - l10 * s00
        y2 = s11 - l20 * s00 - l21 * y1
        c2 = y2 / d2
        c1 = y1 / d1 - l21 * c2
        c0 = s00 / m00 - l10 * c1 - l20 * c2
        e0 = 1.0 - SHIFT * c0
        e1 = c0 + SHIFT * c1
        copies = []
        cuts = [(a, pl.ds(4 * g.rows * b, 4 * g.rows)) for a in range(4) for b in range(4 // 4)]
        rows = [pl.ds(4 * g.rows * i, 4 * g.rows) for i in range(len(cuts))]
        for n, (to, at) in enumerate(zip(cuts, rows)):
            solution_ref[to] = x_ref[to] + (c0 * z0[at] + (c1 * z1[at] + c2 * z2[at]))
            copies.append(pltpu.make_async_copy(solution_ref.at[to], solution_hbm.at[to], sems.at[n]))
            copies[-1].start()
        restore(g, [v_ref], [v3], matrix[...], buffer)
        for n, (to, at) in enumerate(zip(cuts, rows)):
            residual_ref[to] = diag[at] * (e0 * z0[at] - (e1 * z1[at] + c1 * z2[at])) - c2 * v3[at]
            copies.append(pltpu.make_async_copy(residual_ref.at[to], residual_hbm.at[to], sems.at[len(cuts) + n]))
            copies[-1].start()
        for copy in copies:
            copy.wait()

    return body


def swaps(count, parity):
    pairs = []
    for i in range(count):
        step = 1 if i % 2 == parity else -1
        pairs.append((i, (i + step) % count))
    return pairs


VMEM = pl.BlockSpec(memory_space=pltpu.VMEM)
HBM = pl.BlockSpec(memory_space=pltpu.HBM)
MIB = 1024 * 1024


def call(body, args, outs, scratch=(), limit=6, in_specs=None, out_specs=None, aliases=None, flops=1000000):
    return pl.pallas_call(
        body,
        in_specs=in_specs or [VMEM] * len(args),
        out_specs=out_specs or [VMEM] * len(outs),
        out_shape=[jax.ShapeDtypeStruct(s, t) for s, t in outs],
        scratch_shapes=list(scratch),
        input_output_aliases=aliases or {},
        cost_estimate=pl.CostEstimate(flops=flops, bytes_accessed=1000000, transcendentals=0),
        compiler_params=pltpu.CompilerParams(vmem_limit_bytes=limit * MIB),
    )(*args)


def steps(source_term, initial_guess, metric):
    count_x, count_r, count_y = metric.shape[1:]
    assert count_x == 1 and count_r == ROWS and count_y % LANES == 0
    g = Shape(count_r, count_y)
    nx, nr = lax.axis_size("group"), lax.axis_size("rad")
    assert nx % 2 == 0 and nr % 2 == 0
    full = ((16 * count_r, 4 * count_y), F32)
    plane = ((4 * count_r, 4 * count_y), F32)
    edge = ((16, count_y), F32)
    natural = (initial_guess.shape, F32)

    def exchange(p1, p2, p3, p4):
        sends = ((p1, "group", nx, 0), (p2, "group", nx, 1), (p3, "rad", nr, 0), (p4, "rad", nr, 1))
        got = []
        for value, axis, count, parity in sends:
            got.append(lax.ppermute(value, axis, swaps(count, parity)))
        return tuple(got)

    guess = pltpu.with_memory_space_constraint(initial_guess, pltpu.HBM)
    x0, m0, p1, p2, p3, p4, corner = call(
        start_kernel(g),
        (guess, pltpu.with_memory_space_constraint(metric, pltpu.HBM)),
        [natural, (metric.shape, F32)]
        + [((5 * count_r, 4 * count_y), F32)] * 2 + [((8, 4 * count_y), F32)] * 2 + [((8, count_y), F32)],
        [pltpu.SemaphoreType.DMA((17,))],
        in_specs=[HBM, HBM],
    )
    got = exchange(p1, p2, p3, p4)
    diagonal = [
        (i * nr + j, ((i + 1) % nx) * nr + (j + 1) % nr) for i in range(nx) for j in range(nr)
    ]
    corner = lax.ppermute(corner, ("group", "rad"), diagonal)
    matrix = ((4 * LANES, 4 * LANES), BF16)
    tiles = pltpu.VMEM((4 * g.halves, 16 * count_r, LANES), F32)
    slim = ((16 * count_r, count_y), F32)
    xd, sd, matrix, *lines = call(
        arrange_kernel(g),
        (x0, source_term),
        [full, full, matrix, full, full, plane, full, slim],
        [tiles],
    )
    outs = [plane, plane, plane, plane, ((16 * count_r, count_y), F32), full, full]
    outs += [plane, plane, edge, edge]
    cx, cxp, cr, crp, cy, inv, z0, *send = call(
        first_kernel(g),
        (xd, sd, *lines, m0, matrix, *got, corner),
        outs,
        [pltpu.VMEM((8 * count_r, 4 * count_y), F32), pltpu.VMEM((16, 4 * count_y), F32), pltpu.VMEM((count_y // 32, 8 * count_r, LANES), F32)],
    )

    def inner(many, with_diagonal, earlier=()):
        rows = count_r if earlier else count_r * len(many)
        return call(
            inner_kernel(g, len(many), with_diagonal, len(earlier)),
            (cx, cxp, cr, crp, cy, inv, matrix, *many, *earlier),
            [full, ((rows, LANES), F32), full] + [full] * with_diagonal,
            [pltpu.VMEM(*full)] * with_diagonal + [tiles],
        )

    def step(vloc, got, earlier, pulls):
        z, *send = call(
            next_kernel(g, pulls),
            (vloc, cx, cr, inv, *got, *earlier),
            [full, plane, plane, edge, edge],
        )
        return z, send

    got = exchange(*send)
    vloc, d0, z0_n, diag_n = inner((z0,), True)
    z1, send = step(vloc, got, (z0,), (SHIFT,))
    got = exchange(*send)
    vloc, d1, z1_n = inner((z0, z1), False)
    z2, send = step(vloc, got, (z1,), (SHIFT,))
    got = exchange(*send)
    vloc, dots, z2_n = inner((z1, z2), False, (d0, d1))
    v3, message = call(
        last_kernel(g, nx * nr),
        (vloc, cx, cr, z2, *got, dots),
        [full, ((nx * nr, LANES), F32)],
    )
    sums = lax.all_to_all(message, ("group", "rad"), 0, 0, tiled=True)
    return tuple(
        call(
            finish_kernel(g),
            (sums, x0, diag_n, z0_n, z1_n, z2_n, v3, matrix),
            [natural, natural],
            [pltpu.VMEM(*natural)] * 2 + [pltpu.VMEM(*full), tiles, pltpu.SemaphoreType.DMA((8,))],
            out_specs=[HBM, HBM],
        )
    )


def solution(mesh):
    in_specs = (P("group", "rad", None), P("group", "rad", None), P(None, "group", "rad", None))
    out_specs = (P("group", "rad", None), P("group", "rad", None))
    return jax.shard_map(steps, mesh=mesh, in_specs=in_specs, out_specs=out_specs, check_vma=False)
```
